32 devices in a mesh: sims: 4 (over x, core), blk: 8 (over z, y).
Axes of the slice: x: 2, y: 2, z: 4, core: 2. Of those that a mesh axis runs over, the one named last changes fastest.
Arguments:
- sim_alm: bfloat16 [1536, 16, 2, 1536], P('blk', 'sims'), may hold values from -6 to 6
- t_filter: float32 [1536], replicated, may hold values from 0.0006510417 to 0.00390625
- wiener_filter: float32 [1536], replicated, may hold values from 8.477105e-07 to 5.086263e-06
- colatitude: float32 [16], replicated, may hold values from 1.18672 to 1.51328, as said below
- legendre: bfloat16 [1536, 1536, 16], P('blk'), may hold values from -2 to 2, as said below
- pixel_mask: int32 [16, 4096], P('blk'), may hold values 0 or 1
Outputs:
- field_sum: float32 [1536, 2, 1536], P('blk', None, 'sims')
- spectra: float32 [16, 2, 1536], P('sims')
The draws below stay inside these ranges and needn't reach their ends.
Inputs may be any that keep to these rules, and one draw needn't show every extreme that they name: `colatitude`: the colatitudes of 16 cycles in increasing order, about 0.0016 apart, in a band centred between 1.2 and 1.5. legendre[m,l,r] is the orthonormal associated Legendre function of degree l and order m at colatitude[r], zero for l < m, rounded to bfloat16.
All inputs are finite; a program needn't handle non-finite values. No bound on the sum of `pixel_mask` on one device may be relied on, other than what follows from the above.
Results may differ from the reference program's by a relative error of at most 0.006.
The reference program's roundings to bfloat16 on the way (of `coefs`, `cycle_coefs`, `fourier`, `flow_maps`, `mode_coefs` and `tilted`) count: a program that leaves them out, or rounds other values in their place, can miss the bound.
Values may be sent and summed in bfloat16 or wider, within the bound.
A program may use at most 192 MiB of HBM per device.

```python
import math
import jax
import jax.numpy as jnp
from jax import lax

L = 1536
NPHI = 4096
CYCLES = 16
NSIM = 16


def cycle_angles(key):
    jitter = jax.random.uniform(jax.random.fold_in(key, 11), (CYCLES,), jnp.float32, -0.3, 0.3)
    center = jax.random.uniform(jax.random.fold_in(key, 17), (), jnp.float32, 1.2, 1.5)
    spacing = jnp.arange(CYCLES, dtype=jnp.float32) + 0.5 - CYCLES / 2.0 + jitter
    return center + 0.0016 * spacing


def draw_colatitude(key, part):
    return cycle_angles(key)


def draw_legendre(key, part):
    angles = cycle_angles(key)
    cosine = jnp.cos(angles)[None, :]
    log_sine = jnp.log(jnp.sin(angles))[None, :]
    orders = jnp.arange(L, dtype=jnp.float32)[:, None]
    counting = jnp.arange(1, L, dtype=jnp.float32)
    halves = jnp.log((2.0 * counting - 1.0) / (2.0 * counting))
    running = jnp.concatenate([jnp.zeros((1,), jnp.float32), jnp.cumsum(halves)])[:, None]
    diagonal = jnp.exp(0.5 * jnp.log((2.0 * orders + 1.0) / (4.0 * math.pi)) + 0.5 * running + orders * log_sine)

    def advance(state_pair, degree):
        previous, older = state_pair
        ratio_now = jnp.sqrt(jnp.maximum(4.0 * degree * degree - 1.0, 1.0) / jnp.maximum(degree * degree - orders * orders, 1.0))
        lower_degree = degree - 1.0
        ratio_before = jnp.sqrt(jnp.maximum(4.0 * lower_degree * lower_degree - 1.0, 1.0) / jnp.maximum(lower_degree * lower_degree - orders * orders, 1.0))
        general = ratio_now * (cosine * previous - older / ratio_before)
        current = jnp.where(degree == orders, diagonal, jnp.where(degree > orders, general, 0.0))
        return ((current, previous), current.astype(jnp.bfloat16))
    start = jnp.zeros((L, CYCLES), jnp.float32)
    final_state, stacked_rows = lax.scan(advance, (start, start), jnp.arange(L, dtype=jnp.float32))
    return jnp.transpose(stacked_rows, (1, 0, 2))


def with_ends(values, key, low, high):
    longest = values.shape.index(max(values.shape))
    spots = []
    for shift in (0, 1):
        where = [jax.random.randint(jax.random.fold_in(key, axis), (), 0, length) for axis, length in enumerate(values.shape)]
        where[longest] = (where[longest] + shift) % values.shape[longest]
        spots.append(tuple(where))
    return values.at[spots[0]].set(low).at[spots[1]].set(high)


def steps_of(rng, dims, shards, smallest, top_value):
    factor_of = 1.0
    for dim, shards_of in shards:
        steps = jax.random.uniform(jax.random.fold_in(jax.random.fold_in(rng, 6), dim), (shards_of,), jnp.float32, smallest / len(shards), top_value / len(shards))
        factor_of = factor_of * jnp.repeat(jnp.exp(steps), dims[dim] // shards_of).reshape((-1,) + (1,) * (len(dims) - 1 - dim))
    return factor_of


def scatter_about(stream_key, shape, deviation, most, cuts=(), kind=jnp.bfloat16):
    drawn = deviation * jax.random.normal(stream_key, shape, jnp.float32)
    if cuts:
        drawn = drawn * steps_of(stream_key, shape, cuts, -0.22, 0.18)
    return jnp.clip(drawn, -most, most).astype(kind)


def setup_inputs(seed: int = 0) -> dict:
    splits = jax.random.split(jax.random.key(seed), 7)
    sim_alm = scatter_about(splits[0], (L, NSIM, 2, L), 1.0, 6.0, ((0, 8), (1, 4)))
    t_filter = jnp.clip(jnp.exp(jax.random.uniform(splits[1], (L,), jnp.float32, math.log(0.0006510417), math.log(0.00390625))), 0.0006510417, 0.00390625)
    wiener_filter = jnp.clip(jnp.exp(jax.random.uniform(splits[2], (L,), jnp.float32, math.log(8.477105097881577e-07), math.log(5.086263172415784e-06))), 8.477105097881577e-07, 5.086263172415784e-06)
    colatitude = draw_colatitude(jax.random.fold_in(splits[6], 71), 0)
    legendre = draw_legendre(jax.random.fold_in(splits[6], 71), 0)
    pixel_mask = with_ends((jax.random.randint(splits[5], (CYCLES, NPHI), 0, 5) < 4).astype(jnp.int32), jax.random.fold_in(splits[5], 1), 0, 1)
    return {"sim_alm": sim_alm, "t_filter": t_filter, "wiener_filter": wiener_filter, "colatitude": colatitude, "legendre": legendre, "pixel_mask": pixel_mask}


def ladder(degree, orders):
    numerator = (2.0 * degree + 1.0) * (degree * degree - orders * orders)
    denominator = jnp.maximum(2.0 * degree - 1.0, 1.0)
    return jnp.where(degree > orders, jnp.sqrt(jnp.maximum(numerator, 0.0) / denominator), 0.0)

def fourier_table(mode_count, pixels):
    mode_ids = jnp.arange(mode_count, dtype=jnp.int32)[:, None]
    pixel_ids = jnp.arange(pixels, dtype=jnp.int32)[None, :]
    phases = 2.0 * math.pi / pixels * (mode_ids * pixel_ids % pixels).astype(jnp.float32)
    return jnp.stack([jnp.cos(phases).astype(jnp.bfloat16), (-jnp.sin(phases)).astype(jnp.bfloat16)], axis=1)

def reference(sim_alm, t_filter, wiener_filter, colatitude, legendre, pixel_mask):
    highest = lax.Precision.HIGHEST
    degree = jnp.arange(L, dtype=jnp.float32)
    orders = jnp.arange(L, dtype=jnp.float32)
    ladder_steps = ladder(degree[None, :], orders[:, None])
    lookup = legendre.astype(jnp.float32)
    fourier = fourier_table(L, NPHI).astype(jnp.float32)
    mode_weight = jnp.where(orders > 0, 2.0, 1.0)
    mode_weight_half = mode_weight.astype(jnp.bfloat16)
    cotangent = jnp.cos(colatitude) / jnp.sin(colatitude)
    cosecant = 1.0 / jnp.sin(colatitude)
    tilt_factor = jnp.cos(colatitude)
    pixel_weight = pixel_mask.astype(jnp.float32)

    def one_sim(coefficients):
        values = coefficients.astype(jnp.float32)
        weighted = wiener_filter * values
        raised = ladder_steps[:, None, :] * weighted
        lowered = jnp.concatenate([raised[..., 1:], jnp.zeros_like(raised[..., :1])], axis=-1)
        coefs = jnp.stack([t_filter * values, weighted, degree * weighted, lowered], axis=1).astype(jnp.bfloat16)
        legsum = jnp.einsum('mkcl,mlr->mkcr', coefs.astype(jnp.float32), lookup, precision=highest)
        rotated = jnp.stack([-legsum[:, 1, 1], legsum[:, 1, 0]], axis=1) * (orders[:, None, None] * cosecant)
        slopes = cotangent * legsum[:, 2] - cosecant * legsum[:, 3]
        cycle_coefs = jnp.stack([legsum[:, 0], rotated, slopes], axis=1).astype(jnp.bfloat16)
        scaled = cycle_coefs * mode_weight_half[:, None, None, None]
        cycle_maps = jnp.einsum('mqcr,mcj->qrj', scaled.astype(jnp.float32), fourier, precision=highest)
        product = pixel_weight * cycle_maps[0]
        flow_maps = jnp.stack([product * cycle_maps[2], product * cycle_maps[1]]).astype(jnp.bfloat16)
        mode_coefs = (jnp.einsum('prj,mcj->mpcr', flow_maps.astype(jnp.float32), fourier, precision=highest) * (2.0 * math.pi / NPHI)).astype(jnp.bfloat16)
        tilted = (tilt_factor * mode_coefs[:, 0].astype(jnp.float32)).astype(jnp.bfloat16)
        stacked = jnp.stack([tilted, mode_coefs[:, 0], mode_coefs[:, 1]], axis=1)
        projected = jnp.einsum('mkcr,mlr->mkcl', stacked.astype(jnp.float32), lookup, precision=highest)
        shifted = jnp.concatenate([jnp.zeros_like(projected[:, 1, :, :1]), projected[:, 1, :, :-1]], axis=-1)
        real_part = degree * projected[:, 0, 0] - ladder_steps * shifted[:, 0] + orders[:, None] * projected[:, 2, 1]
        imag_part = degree * projected[:, 0, 1] - ladder_steps * shifted[:, 1] - orders[:, None] * projected[:, 2, 0]
        return jnp.stack([real_part, imag_part], axis=1) / L
    estimates = lax.map(one_sim, jnp.moveaxis(sim_alm, 1, 0))
    field_sum = lax.optimization_barrier(jnp.sum(estimates, axis=0))
    residual = estimates - field_sum / NSIM
    partner = residual.reshape(NSIM // 2, 2, L, 2, L)[:, ::-1].reshape(residual.shape)
    auto_power = lax.optimization_barrier(jnp.sum(residual * residual, axis=2))
    cross_power = lax.optimization_barrier(jnp.sum(residual * partner, axis=2))
    spectra = jnp.stack([jnp.einsum('m,sml->sl', mode_weight, auto_power, precision=highest), jnp.einsum('m,sml->sl', mode_weight, cross_power, precision=highest)], axis=1)
    spectra = spectra / (2.0 * degree + 1.0)
    return (field_sum, spectra)
```

```python
import functools
import math

import jax
import jax.numpy as jnp
import numpy as np
from jax import lax
from jax.experimental import pallas as pl
from jax.experimental.pallas import tpu as pltpu
from jax.sharding import PartitionSpec as P

F32 = jnp.float32
BF16 = jnp.bfloat16
LANES = 128
SLOTS = 32
GROUP = 8
MESH = pl.DeviceIdType.MESH
NT = (((1,), (1,)), ((), ()))
SIGNS = ((1, 1, 1, 1), (1, -1, -1, 1), (1, -1, 1, -1), (1, 1, -1, -1))


def chunk_of(orders):
    best = 0
    for size in range(GROUP, 2 * SLOTS + 1, GROUP):
        if orders % size == 0:
            best = size
    assert best > 0
    return best


def image_signs(img):
    part = lax.broadcasted_iota(jnp.int32, (1, LANES), 1) // SLOTS
    sign = jnp.ones((1, LANES), F32)
    for k in range(4):
        if SIGNS[img][k] < 0:
            sign = jnp.where(part == k, -1.0, sign)
    return sign


def kernel(
    alm_hbm, leg_hbm, fine_hbm, coarse_hbm, filt, ang, mask,
    field_out, spec_out,
    alm, leg, fine, coarse, lad, raise8, sums, send_x, recv_x, table, send_y, recv_y, gath_y,
    cols, fcols, unpacked, funpacked, est, acc, box, parts,
    sem_in, sem_c, sx, rx, sy, ry, sg, rg, ss, rs,
    *, chunk, scale,
):
    orders, sims, _, degrees = alm.shape
    cycles = leg.shape[1]
    blocks = recv_y.shape[0]
    chunks = recv_y.shape[1]
    groups = gath_y.shape[0]
    steps = orders // GROUP
    nblk = blocks * chunks
    width = table.shape[2]
    rows = 2 * sims
    me = lax.axis_index("blk")
    mine = lax.axis_index("sims")
    first = me * orders

    barrier = pltpu.get_barrier_semaphore()

    def greet_blk(o, carry):
        pl.semaphore_signal(
            barrier, inc=1, device_id={"blk": lax.rem(me + o, blocks)}, device_id_type=MESH
        )
        return carry

    def greet_sims(o, carry):
        pl.semaphore_signal(
            barrier, inc=1, device_id={"sims": lax.rem(mine + o, groups)}, device_id_type=MESH
        )
        return carry

    lax.fori_loop(1, blocks, greet_blk, 0)
    lax.fori_loop(1, groups, greet_sims, 0)

    def load_alm(n):
        part = pl.ds(n * GROUP, GROUP)
        return pltpu.make_async_copy(alm_hbm.at[part], alm.at[part], sem_in.at[n, 0])

    def load_leg(n):
        part = pl.ds(n * GROUP, GROUP)
        return pltpu.make_async_copy(leg_hbm.at[part], leg.at[part], sem_in.at[n, 1])

    load_fine = pltpu.make_async_copy(fine_hbm, fine, sem_c.at[0])
    load_coarse = pltpu.make_async_copy(coarse_hbm, coarse, sem_c.at[1])
    load_alm(0).start()
    load_leg(0).start()
    load_fine.start()
    load_coarse.start()

    def start_loads(n, carry):
        load_alm(n).start()
        load_leg(n).start()
        return carry

    lax.fori_loop(1, steps, start_loads, 0)

    degree = lax.broadcasted_iota(jnp.int32, (1, degrees), 1).astype(F32)
    lane = lax.broadcasted_iota(jnp.int32, (1, LANES), 1)
    slot = lane % SLOTS
    parity = (lane // SLOTS) % 2
    half = lane // (2 * SLOTS)
    row8 = lax.broadcasted_iota(jnp.int32, (rows, LANES), 0)
    per = -(-nblk // steps)

    def table_block(n):
        table[n] = (
            fine[0] * coarse[0, pl.ds(n, 1), :] + fine[1] * coarse[1, pl.ds(n, 1), :]
        ).astype(BF16)

    for t in range(chunks):

        def step(i, carry):
            n = t * (chunk // GROUP) + i
            load_alm(n).wait()
            load_leg(n).wait()
            order = (
                lax.broadcasted_iota(jnp.int32, (GROUP, 1), 0) + (first + n * GROUP)
            ).astype(F32)
            square = (degree * degree - order * order) * filt[3:4, :]
            ladder = jnp.where(degree > order, jnp.sqrt(jnp.maximum(square, 0.0)), 0.0)
            lad[pl.ds(n * GROUP, GROUP), :] = ladder * (1.0 / degrees)
            raise8[...] = ladder * filt[1:2, :]
            for u in range(GROUP):
                values = alm[n * GROUP + u].astype(F32).reshape(rows, degrees)
                raised = raise8[u : u + 1, :] * values
                lowered = jnp.where(
                    degree < degrees - 1, pltpu.roll(raised, degrees - 1, 1), 0.0
                )
                coefs = jnp.concatenate(
                    [filt[0:1, :] * values, filt[1:2, :] * values, filt[2:3, :] * values, lowered],
                    axis=0,
                ).astype(BF16)
                sums[pl.ds((i * GROUP + u) * cycles, cycles), 0 : 4 * rows] = lax.dot_general(
                    leg[n * GROUP + u], coefs, NT, preferred_element_type=F32
                )
            if per == 1:

                @pl.when(n == 0)
                def _():
                    load_fine.wait()
                    load_coarse.wait()

                table_block(n)
            return carry

        lax.fori_loop(0, chunk // GROUP, step, 0)

        def message(dest):
            pieces = []
            for r in range(2):
                for p in range(2):
                    pieces.append(
                        sums[pl.ds(p * cycles + 2 * dest + r, SLOTS, stride=2 * cycles), :]
                    )
            turned = jnp.concatenate(pieces, axis=0).T
            order_int = first + t * chunk + 2 * slot + parity
            order = order_int.astype(F32)
            cot = jnp.where(half == 0, ang[0, 2 * dest], ang[0, 2 * dest + 1])
            csc = jnp.where(half == 0, ang[1, 2 * dest], ang[1, 2 * dest + 1])
            wave = turned[rows : 2 * rows]
            odd_row = row8 % 2
            rotated = jnp.where(
                odd_row == 0, -pltpu.roll(wave, rows - 1, 0), pltpu.roll(wave, 1, 0)
            ) * (csc * order)
            slopes = cot * turned[2 * rows : 3 * rows] - csc * turned[3 * rows : 4 * rows]
            weight = jnp.where(order_int > 0, 2.0, 1.0)
            out = []
            for value in (turned[:rows], rotated, slopes):
                value = jnp.where(slot < chunk // 2, value * weight, 0.0)
                swapped = pltpu.roll(value, 2 * SLOTS, 1)
                out.append(
                    jnp.where(
                        odd_row == half,
                        value,
                        jnp.where(
                            odd_row == 1, pltpu.roll(swapped, 1, 0), pltpu.roll(swapped, rows - 1, 0)
                        ),
                    )
                )
            return jnp.concatenate(out, axis=0).astype(BF16)

        if t == 0:
            pl.semaphore_wait(barrier, blocks - 1 + groups - 1)

        def send(o, carry):
            dest = lax.rem(me + o, blocks)
            send_x[t, dest] = message(dest)
            pltpu.make_async_remote_copy(
                src_ref=send_x.at[t, dest],
                dst_ref=recv_x.at[me, t],
                send_sem=sx.at[t, dest],
                recv_sem=rx.at[me, t],
                device_id={"blk": dest},
                device_id_type=MESH,
            ).start()
            return carry

        lax.fori_loop(1, blocks, send, 0)
        recv_x[me, t] = message(me)

    if per > 1:
        load_fine.wait()
        load_coarse.wait()

        def fill(n, carry):
            table_block(n)
            return carry

        lax.fori_loop(0, nblk, fill, 0)

    def copy_x(t, dest, source):
        return pltpu.make_async_remote_copy(
            src_ref=send_x.at[t, dest],
            dst_ref=recv_x.at[source, t],
            send_sem=sx.at[t, dest],
            recv_sem=rx.at[source, t],
            device_id={"blk": dest},
            device_id_type=MESH,
        )

    def wait_x(o, carry):
        other = lax.rem(me + o, blocks)
        for t in range(chunks):
            copy_x(t, other, other).wait_recv()
        return carry

    lax.fori_loop(1, blocks, wait_x, 0)

    pieces = recv_x[...].reshape(nblk, 3 * rows, LANES)
    images = []
    for img in range(4):
        sign = image_signs(img).astype(BF16)
        images.append(
            jnp.concatenate([pieces[n] * sign for n in range(nblk)], axis=1)
        )
    stacked = jnp.concatenate(images, axis=0)
    maps = jnp.dot(
        stacked, table[...].reshape(nblk * LANES, width), preferred_element_type=F32
    )
    flows = []
    for img in range(4):
        base = img * 3 * rows
        product = mask[img] * maps[base : base + rows]
        flows.append(product * maps[base + 2 * rows : base + 3 * rows])
        flows.append(product * maps[base + rows : base + 2 * rows])
    flows = jnp.concatenate(flows, axis=0).astype(BF16)
    for n in range(nblk):
        part = lax.dot_general(flows, table[n], NT, preferred_element_type=F32)
        total = part[: 2 * rows]
        for img in range(1, 4):
            total = total + part[2 * rows * img : 2 * rows * (img + 1)] * image_signs(img)
        send_y[n // chunks, n % chunks] = (total * scale).astype(BF16)

    def copy_y(dest, source):
        return pltpu.make_async_remote_copy(
            src_ref=send_y.at[dest],
            dst_ref=recv_y.at[source],
            send_sem=sy.at[dest],
            recv_sem=ry.at[source],
            device_id={"blk": dest},
            device_id_type=MESH,
        )

    def put_y(o, carry):
        copy_y(lax.rem(me + o, blocks), me).start()
        return carry

    lax.fori_loop(1, blocks, put_y, 0)
    recv_y[me] = send_y[me]

    def copy_g(o, source, group):
        return pltpu.make_async_remote_copy(
            src_ref=recv_y.at[source],
            dst_ref=gath_y.at[group, source],
            send_sem=sg.at[o, source],
            recv_sem=rg.at[group, source],
            device_id={"sims": lax.rem(mine + o, groups)},
            device_id_type=MESH,
        )

    def spread(source):
        for o in range(1, groups):
            copy_g(o, source, mine).start()

    spread(me)

    def pass_y(o, carry):
        source = lax.rem(me + o, blocks)
        copy_y(source, source).wait_recv()
        spread(source)
        return carry

    lax.fori_loop(1, blocks, pass_y, 0)

    wide = blocks * 2 * rows
    spot = lax.broadcasted_iota(jnp.int32, (rows, wide), 1)
    srow = lax.broadcasted_iota(jnp.int32, (rows, wide), 0)
    same = (spot // 2) % sims == srow % sims
    flow = (spot // rows) % 2
    mask_first = jnp.where(same & (flow == 0), 1.0, 0.0)
    mask_second = jnp.where(same & (flow == 1), jnp.where(srow < sims, 1.0, -1.0), 0.0)
    low_rows = srow < sims
    pick_row = lax.broadcasted_iota(jnp.int32, (wide, cycles), 0)
    pick_col = lax.broadcasted_iota(jnp.int32, (wide, cycles), 1)
    pick = jnp.where(
        (pick_row // (2 * rows)) * 2 + pick_row % 2 == pick_col, 1.0, 0.0
    ).astype(BF16)
    for t in range(chunks):
        cols[t] = recv_y[:, t].astype(F32).reshape(wide, LANES).T
    tilt_row = filt[7:8, 0:cycles]

    def unpack(j, carry):
        base = (j // 4) * LANES + (j % 4) * GROUP
        tiles = []
        for u in range(GROUP):
            at = (j // 8)
            line = (j % 8) * GROUP + u
            real = cols[at, pl.ds(line, 1), :]
            imag = cols[at, pl.ds(line + 2 * SLOTS, 1), :]
            tiles.append(jnp.where(low_rows, real, imag) * mask_first)
            tiles.append(jnp.where(low_rows, imag, real) * mask_second)
        out = jnp.dot(
            jnp.concatenate(tiles, axis=0).astype(BF16), pick, preferred_element_type=F32
        )
        for u in range(GROUP):
            one = out[2 * rows * u : 2 * rows * u + rows]
            two = out[2 * rows * u + rows : 2 * rows * (u + 1)]
            unpacked[j * GROUP + u] = jnp.concatenate(
                [(tilt_row * one).astype(BF16).astype(F32), one, two], axis=0
            )
        return carry

    lax.fori_loop(0, chunks * 8, unpack, 0)

    def combine(sums3, ladder, order):
        shifted = jnp.where(degree > 0, pltpu.roll(sums3[rows : 2 * rows], 1, 1), 0.0)
        return (
            filt[4:5, :] * sums3[:rows]
            - ladder * shifted
            + (order * (1.0 / degrees)) * sums3[2 * rows : 3 * rows]
        )

    def place(n):
        t = n // chunk
        rest = n % chunk
        return t * 2 * SLOTS + (rest % 2) * SLOTS + rest // 2

    def project(i, carry):
        for u in range(GROUP):
            n = i * GROUP + u
            order = (first + n).astype(F32)
            sums3 = jnp.dot(
                unpacked[place(n)].astype(BF16), leg[n], preferred_element_type=F32
            )
            est[n] = combine(sums3, lad[pl.ds(n, 1), :], order)
        return carry

    lax.fori_loop(0, steps, project, 0)

    def wait_g(source, carry):
        for o in range(1, groups):
            copy_g(o, source, lax.rem(mine + o, groups)).wait_recv()
        return carry

    lax.fori_loop(0, blocks, wait_g, 0)

    def gather_sums(b, carry):
        cos_rows = jnp.where(row8 % 2 == 0, ang[2, 2 * b], ang[2, 2 * b + 1])
        for t in range(chunks):
            one = jnp.zeros((rows, LANES), F32)
            two = jnp.zeros((rows, LANES), F32)
            tilted = jnp.zeros((rows, LANES), F32)
            for o in range(groups):
                if o == 0:
                    value = recv_y[b, t].astype(F32)
                else:
                    value = gath_y[lax.rem(mine + o, groups), b, t].astype(F32)
                one = one + value[:rows]
                two = two + value[rows:]
                tilted = tilted + (cos_rows * value[:rows]).astype(BF16).astype(F32)
            out = []
            for value in (one, two, tilted):
                value = value + pltpu.roll(value, 2, 0)
                out.append(value + pltpu.roll(value, 4, 0))
            parts[b, t] = jnp.concatenate(out + [jnp.zeros_like(one)], axis=0)
        return carry

    lax.fori_loop(0, blocks, gather_sums, 0)
    for t in range(chunks):
        for k in range(2):
            fcols[t, k] = parts[:, t, 2 * rows * k : 2 * rows * (k + 1), :].reshape(wide, LANES).T
    none = jnp.zeros_like(pick)
    pick2 = jnp.concatenate(
        [jnp.concatenate([pick, none], axis=1), jnp.concatenate([none, pick], axis=1)], axis=0
    )

    def funpack(j, carry):
        tiles = []
        at = j // 8
        for u in range(GROUP):
            line = (j % 8) * GROUP + u
            real = fcols[at, 0, pl.ds(line, 1), :]
            imag = fcols[at, 0, pl.ds(line + 2 * SLOTS, 1), :]
            treal = fcols[at, 1, pl.ds(line, 1), :]
            timag = fcols[at, 1, pl.ds(line + 2 * SLOTS, 1), :]
            tiles.append(jnp.where(low_rows, treal, timag) * mask_first)
            tiles.append(jnp.where(low_rows, real, imag) * mask_first)
            tiles.append(jnp.where(low_rows, imag, real) * mask_second)
        whole = jnp.concatenate(tiles, axis=0)
        upper = whole.astype(BF16)
        lower = (whole - upper.astype(F32)).astype(BF16)
        out = jnp.dot(
            jnp.concatenate([upper, lower], axis=1), pick2, preferred_element_type=F32
        )
        for u in range(GROUP):
            funpacked[j * GROUP + u] = out[3 * rows * u : 3 * rows * (u + 1)]
        return carry

    lax.fori_loop(0, chunks * 8, funpack, 0)

    acc[...] = jnp.zeros_like(acc)
    share = degrees // groups

    def finish(i, carry):
        auto = acc[0]
        cross = acc[1]
        for u in range(GROUP):
            n = i * GROUP + u
            order_int = first + n
            order = order_int.astype(F32)
            tile = leg[n]
            sums3 = jnp.dot(
                funpacked[place(n)].astype(BF16),
                jnp.concatenate([tile, tile], axis=0),
                preferred_element_type=F32,
            )
            field = combine(sums3, lad[pl.ds(n, 1), :], order)
            quarter = field[:, 0:share]
            for g in range(1, groups):
                quarter = jnp.where(mine == g, field[:, g * share : (g + 1) * share], quarter)
            field_out[n, 0:1, :] = quarter[0:1]
            field_out[n, 1:2, :] = quarter[sims : sims + 1]
            residual = est[n] - field * (1.0 / (sims * groups))
            weight = jnp.where(order_int > 0, 2.0, 1.0)
            weighted = weight * residual
            auto = auto + weighted * residual
            cross = cross + weighted * pltpu.roll(residual, rows - 1, 0)
        acc[0] = auto
        acc[1] = cross
        return carry

    lax.fori_loop(0, steps, finish, 0)

    wide_row = lax.broadcasted_iota(jnp.int32, (rows, degrees), 0)
    auto = acc[0] + pltpu.roll(acc[0], sims, 0)
    cross = acc[1] + pltpu.roll(acc[1], sims, 0)
    cross = jnp.where(wide_row % 2 == 0, cross, pltpu.roll(cross, 1, 0))
    total = jnp.where(wide_row < sims, auto, cross) * filt[6:7, :]
    spectra = total
    box[blocks] = spectra

    def copy_s(dest, source):
        return pltpu.make_async_remote_copy(
            src_ref=box.at[blocks],
            dst_ref=box.at[source],
            send_sem=ss.at[dest],
            recv_sem=rs.at[source],
            device_id={"blk": dest},
            device_id_type=MESH,
        )

    def put_s(o, carry):
        copy_s(lax.rem(me + o, blocks), me).start()
        return carry

    lax.fori_loop(1, blocks, put_s, 0)
    box[me] = spectra

    def wait_s(o, carry):
        other = lax.rem(me + o, blocks)
        copy_s(other, other).wait_recv()
        return carry

    lax.fori_loop(1, blocks, wait_s, 0)

    def add_s(b, value):
        return value + box[b]

    result = lax.fori_loop(0, blocks, add_s, jnp.zeros_like(spectra))
    for s in range(sims):
        spec_out[s, 0:1, :] = result[s : s + 1]
        spec_out[s, 1:2, :] = result[sims + s : sims + s + 1]

    def drain(o, carry):
        other = lax.rem(me + o, blocks)
        for t in range(chunks):
            copy_x(t, other, other).wait_send()
        copy_y(other, other).wait_send()
        copy_s(other, other).wait_send()
        return carry

    lax.fori_loop(1, blocks, drain, 0)

    def drain_g(source, carry):
        for o in range(1, groups):
            copy_g(o, source, mine).wait_send()
        return carry

    lax.fori_loop(0, blocks, drain_g, 0)


def angle_tables(blocks, chunks, chunk, pixels, width):
    pixel = np.arange(width)

    def waves(orders):
        turn = 2.0 * np.pi / pixels * ((orders[:, None] * pixel[None, :]) % pixels)
        return np.cos(turn), np.sin(turn)

    even = waves(2 * np.arange(SLOTS))
    odd = waves(2 * np.arange(SLOTS) + 1)
    fine = np.stack(
        [
            np.concatenate([even[0], odd[0], -even[1], -odd[1]]),
            np.concatenate([-even[1], -odd[1], -even[0], -odd[0]]),
        ]
    )
    coarse = np.stack(waves(chunk * np.arange(blocks * chunks)))
    return fine.astype(np.float32), coarse.astype(np.float32)


def per_device(sim_alm, t_filter, wiener_filter, colatitude, legendre, pixel_mask):
    orders, sims, parts, degrees = sim_alm.shape
    cycles = legendre.shape[2]
    pixels = pixel_mask.shape[1]
    blocks = lax.axis_size("blk")
    groups = lax.axis_size("sims")
    rows = sims * parts
    assert rows == 8 and cycles == 2 * blocks
    chunk = chunk_of(orders)
    chunks = orders // chunk
    nblk = blocks * chunks
    quarter = pixels // 4
    width = quarter + LANES
    steps = orders // GROUP

    fine, coarse = angle_tables(blocks, chunks, chunk, pixels, width)
    degree = jnp.arange(degrees, dtype=F32)
    ratio = (2.0 * degree + 1.0) / jnp.maximum(2.0 * degree - 1.0, 1.0)
    tilt = jnp.cos(colatitude)
    filters = jnp.stack(
        [
            t_filter,
            wiener_filter,
            degree * wiener_filter,
            ratio,
            degree * (1.0 / degrees),
            degree,
            1.0 / (2.0 * degree + 1.0),
            jnp.pad(tilt, (0, degrees - cycles)),
        ]
    )
    angles = jnp.stack([tilt / jnp.sin(colatitude), 1.0 / jnp.sin(colatitude), tilt])
    seen = pixel_mask.astype(F32)
    gap = jnp.zeros((2, 1), F32)
    tail = jnp.zeros((2, width - quarter - 1), F32)
    flipped = jnp.flip(seen, axis=1)
    images = jnp.stack(
        [
            jnp.concatenate([seen[:, : quarter + 1], tail], axis=1),
            jnp.concatenate([flipped[:, 2 * quarter - 1 : 3 * quarter - 1], gap, tail], axis=1),
            jnp.concatenate([gap, seen[:, 2 * quarter + 1 : 3 * quarter + 1], tail], axis=1),
            jnp.concatenate([gap, flipped[:, : quarter - 1], gap, tail], axis=1),
        ]
    )
    masks = jnp.tile(images, (1, sims, 1))
    leg_rows = jnp.transpose(legendre, (0, 2, 1))

    hbm = pl.BlockSpec(memory_space=pl.ANY)
    vmem = pl.BlockSpec(memory_space=pltpu.VMEM)
    smem = pl.BlockSpec(memory_space=pltpu.SMEM)
    dma = pltpu.SemaphoreType.DMA
    wide = blocks * 2 * rows
    return pl.pallas_call(
        functools.partial(kernel, chunk=chunk, scale=2.0 * math.pi / pixels),
        in_specs=[hbm, hbm, hbm, hbm, vmem, smem, vmem],
        out_specs=[vmem, vmem],
        out_shape=[
            jax.ShapeDtypeStruct((orders, 2, degrees // groups), F32),
            jax.ShapeDtypeStruct((sims, 2, degrees), F32),
        ],
        scratch_shapes=[
            pltpu.VMEM((orders, sims, parts, degrees), BF16),
            pltpu.VMEM((orders, cycles, degrees), BF16),
            pltpu.VMEM((2, LANES, width), F32),
            pltpu.VMEM((2, nblk, width), F32),
            pltpu.VMEM((orders, degrees), F32),
            pltpu.VMEM((GROUP, degrees), F32),
            pltpu.VMEM((2 * SLOTS * cycles, LANES), F32),
            pltpu.VMEM((chunks, blocks, 3 * rows, LANES), BF16),
            pltpu.VMEM((blocks, chunks, 3 * rows, LANES), BF16),
            pltpu.VMEM((nblk, LANES, width), BF16),
            pltpu.VMEM((blocks, chunks, 2 * rows, LANES), BF16),
            pltpu.VMEM((blocks, chunks, 2 * rows, LANES), BF16),
            pltpu.VMEM((groups, blocks, chunks, 2 * rows, LANES), BF16),
            pltpu.VMEM((chunks, LANES, wide), F32),
            pltpu.VMEM((chunks, 2, LANES, wide), F32),
            pltpu.VMEM((chunks * 2 * SLOTS, 3 * rows, cycles), F32),
            pltpu.VMEM((chunks * 2 * SLOTS, 3 * rows, 2 * cycles), F32),
            pltpu.VMEM((orders, rows, degrees), F32),
            pltpu.VMEM((2, rows, degrees), F32),
            pltpu.VMEM((1 + blocks, rows, degrees), F32),
            pltpu.VMEM((blocks, chunks, 4 * rows, LANES), F32),
            dma((steps, 2)),
            dma((2,)),
            dma((chunks, blocks)),
            dma((blocks, chunks)),
            dma((blocks,)),
            dma((blocks,)),
            dma((groups, blocks)),
            dma((groups, blocks)),
            dma((blocks,)),
            dma((blocks,)),
        ],
        compiler_params=pltpu.CompilerParams(
            collective_id=0, has_side_effects=True, vmem_limit_bytes=64 * 1024 * 1024 - 65536 * 2
        ),
        name="lensing",
    )(sim_alm, leg_rows, jnp.asarray(fine), jnp.asarray(coarse), filters, angles, masks)


def solution(mesh):
    placed = (P("blk", "sims", None, None), P(), P(), P(), P("blk", None, None), P("blk", None))
    return jax.shard_map(
        per_device,
        mesh=mesh,
        in_specs=placed,
        out_specs=(P("blk", None, "sims"), P("sims", None, None)),
        check_vma=False,
    )
```

```python
import functools
import math

import jax
import jax.numpy as jnp
import numpy as np
from jax import lax
from jax.experimental import pallas as pl
from jax.experimental.pallas import tpu as pltpu
from jax.sharding import PartitionSpec as P

F32 = jnp.float32
BF16 = jnp.bfloat16
LANES = 128
SLOTS = 32
GROUP = 8
DEPTH = 6
VMEM_LIMIT = 66977792
MESH = pl.DeviceIdType.MESH
NT = (((1,), (1,)), ((), ()))
SIGNS = ((1, 1, 1, 1), (1, -1, -1, 1), (1, -1, 1, -1), (1, 1, -1, -1))


def chunk_of(orders):
    best = 0
    for size in range(GROUP, 2 * SLOTS + 1, GROUP):
        if orders % size == 0:
            best = size
    assert best > 0
    return best


def image_signs(img):
    part = lax.broadcasted_iota(jnp.int32, (1, LANES), 1) // SLOTS
    sign = jnp.ones((1, LANES), F32)
    for k in range(4):
        if SIGNS[img][k] < 0:
            sign = jnp.where(part == k, -1.0, sign)
    return sign


def kernel(
    alm_hbm, leg_hbm, fine_hbm, coarse_hbm, t_filter, w_filter, colatitude, seen,
    field_out, spec_out,
    alm, leg, fine, coarse, filt, ang, mask, lad, raised_rows, sums, send_x, recv_x, table,
    send_y, recv_y, gath_y, cols, fcols, parts, coefs_y, coefs_f, est, field, box,
    sem_in, sem_c, sx, rx, sy, ry, sg, rg, ss, rs,
    *, chunk, scale, pixels,
):
    orders, tiles = alm.shape[:2]
    rows = alm.shape[2]
    sims = rows // 2
    degrees = tiles * LANES
    cycles = leg.shape[1]
    blocks = recv_y.shape[0]
    chunks = recv_y.shape[1]
    groups = gath_y.shape[0]
    steps = orders // GROUP
    per_chunk = chunk // GROUP
    nblk = blocks * chunks
    width = table.shape[2]
    quad = GROUP // 2
    me = lax.axis_index("blk")
    mine = lax.axis_index("sims")
    first = me * orders

    barrier = pltpu.get_barrier_semaphore()

    def greet_blk(o, carry):
        pl.semaphore_signal(
            barrier, inc=1, device_id={"blk": lax.rem(me + o, blocks)}, device_id_type=MESH
        )
        return carry

    def greet_sims(o, carry):
        pl.semaphore_signal(
            barrier, inc=1, device_id={"sims": lax.rem(mine + o, groups)}, device_id_type=MESH
        )
        return carry

    def start_load(n):
        part = pl.ds(n * GROUP, GROUP)
        pltpu.make_async_copy(leg_hbm.at[part], leg.at[part], sem_in.at[n % DEPTH, 0]).start()
        for s in range(sims):
            pltpu.make_async_copy(
                alm_hbm.at[part, s],
                alm.at[part, :, pl.ds(2 * s, 2), :],
                sem_in.at[n % DEPTH, 1],
            ).start()

    def wait_load(n):
        part = pl.ds(n * GROUP, GROUP)
        pltpu.make_async_copy(leg.at[part], leg.at[part], sem_in.at[n % DEPTH, 0]).wait()
        pltpu.make_async_copy(alm.at[part], alm.at[part], sem_in.at[n % DEPTH, 1]).wait()

    load_fine = pltpu.make_async_copy(fine_hbm, fine, sem_c.at[0])
    load_coarse = pltpu.make_async_copy(coarse_hbm, coarse, sem_c.at[1])

    ahead = min(DEPTH, steps)
    for n in range(ahead):
        start_load(n)
    load_fine.start()
    load_coarse.start()
    lax.fori_loop(1, blocks, greet_blk, 0)
    lax.fori_loop(1, groups, greet_sims, 0)

    degree = lax.broadcasted_iota(jnp.int32, (1, degrees), 1).astype(F32)
    lane = lax.broadcasted_iota(jnp.int32, (1, LANES), 1)
    slot = lane % SLOTS
    parity = (lane // SLOTS) % 2
    half = lane // (2 * SLOTS)
    row8 = lax.broadcasted_iota(jnp.int32, (rows, LANES), 0)
    column = lax.broadcasted_iota(jnp.int32, (rows, 1), 0)

    t_row = t_filter[...].reshape(1, degrees)
    w_row = w_filter[...].reshape(1, degrees)
    filt[0:1, :] = t_row
    filt[1:2, :] = w_row
    filt[2:3, :] = degree * w_row
    filt[3:4, :] = (2.0 * degree + 1.0) / jnp.maximum(2.0 * degree - 1.0, 1.0)
    filt[4:5, :] = degree * (1.0 / degrees)
    filt[5:6, :] = 1.0 / (2.0 * degree + 1.0)

    angle = colatitude[...].reshape(1, cycles)
    cosine = jnp.cos(angle)
    cosecant = 1.0 / jnp.sin(angle)
    square_row = lax.broadcasted_iota(jnp.int32, (cycles, cycles), 0)
    square_col = lax.broadcasted_iota(jnp.int32, (cycles, cycles), 1)
    for k, value in enumerate((cosine * cosecant, cosecant, cosine)):
        spread_out = jnp.where(square_row == square_col, value, 0.0)
        ang[k] = jnp.broadcast_to(
            jnp.sum(spread_out, axis=1, keepdims=True), (cycles, LANES)
        )
    tilt_row = jnp.concatenate([cosine] * quad, axis=1)

    quarter = pixels // 4
    both = seen[...].astype(F32)
    both = jnp.where(
        lax.broadcasted_iota(jnp.int32, (rows, pixels), 0) % 2 == 0, both[0:1], both[1:2]
    )
    both = jnp.concatenate([both, jnp.zeros((rows, LANES), F32)], axis=1)
    turn_row = lax.broadcasted_iota(jnp.int32, (2 * LANES, LANES), 0)
    turn_col = lax.broadcasted_iota(jnp.int32, (2 * LANES, LANES), 1)
    turn = jnp.where(turn_row + turn_col == LANES, 1.0, 0.0).astype(BF16)
    half_seen = both.astype(BF16)
    for n in range(width // LANES):
        pixel = lane + n * LANES
        here = slice(n * LANES, (n + 1) * LANES)
        back = pixels // 2 - (n + 1) * LANES
        straight = both[:, n * LANES : (n + 1) * LANES]
        mask[0, :, here] = jnp.where(pixel <= quarter, straight, 0.0)
        mirror = jnp.dot(
            half_seen[:, back : back + 2 * LANES], turn, preferred_element_type=F32
        )
        mask[1, :, here] = jnp.where(pixel < quarter, mirror, 0.0)
        at = pixels // 2 + n * LANES
        mask[2, :, here] = jnp.where(
            (pixel > 0) & (pixel <= quarter), both[:, at : at + LANES], 0.0
        )
        back = pixels - (n + 1) * LANES
        mirror = jnp.dot(
            half_seen[:, back : back + 2 * LANES], turn, preferred_element_type=F32
        )
        mask[3, :, here] = jnp.where((pixel > 0) & (pixel < quarter), mirror, 0.0)

    def quad_orders(n, p):
        return (first + n * GROUP + 2 * (column % quad) + p).astype(F32)

    def copy_x(t, dest, source):
        return pltpu.make_async_remote_copy(
            src_ref=send_x.at[t, dest],
            dst_ref=recv_x.at[source, t],
            send_sem=sx,
            recv_sem=rx,
            device_id={"blk": dest},
            device_id_type=MESH,
        )

    for t in range(chunks):

        def step(i, carry):
            n = t * per_chunk + i
            wait_load(n)

            @pl.when(n + ahead < steps)
            def _():
                start_load(n + ahead)

            for p in range(2):
                order = quad_orders(n, p)
                square = (degree * degree - order * order) * filt[3:4, :]
                ladder = jnp.where(degree > order, jnp.sqrt(jnp.maximum(square, 0.0)), 0.0)
                lad[2 * n + p] = ladder * (1.0 / degrees)
                raised_rows[p] = ladder * filt[1:2, :]
            for u in range(GROUP):
                values = jnp.concatenate(
                    [alm[n * GROUP + u, k].astype(F32) for k in range(tiles)], axis=1
                )
                raised = raised_rows[u % 2, u // 2 : u // 2 + 1, :] * values
                lowered = pltpu.roll(raised, degrees - 1, 1)
                coefs = jnp.concatenate(
                    [filt[0:1, :] * values, filt[1:2, :] * values, filt[2:3, :] * values, lowered],
                    axis=0,
                ).astype(BF16)
                sums[pl.ds((i * GROUP + u) * cycles, cycles), 0 : 4 * rows] = lax.dot_general(
                    leg[n * GROUP + u], coefs, NT, preferred_element_type=F32
                )
            return carry

        lax.fori_loop(0, per_chunk, step, 0)

        def message(dest):
            pieces = []
            for r in range(2):
                for p in range(2):
                    pieces.append(
                        sums[pl.ds(p * cycles + 2 * dest + r, SLOTS, stride=2 * cycles), :]
                    )
            turned = jnp.concatenate(pieces, axis=0).T
            order_int = first + t * chunk + 2 * slot + parity
            order = order_int.astype(F32)
            cot = jnp.where(
                half == 0, ang[0, pl.ds(2 * dest, 1), :], ang[0, pl.ds(2 * dest + 1, 1), :]
            )
            csc = jnp.where(
                half == 0, ang[1, pl.ds(2 * dest, 1), :], ang[1, pl.ds(2 * dest + 1, 1), :]
            )
            wave = turned[rows : 2 * rows]
            odd_row = row8 % 2
            rotated = jnp.where(
                odd_row == 0, -pltpu.roll(wave, rows - 1, 0), pltpu.roll(wave, 1, 0)
            ) * (csc * order)
            slopes = cot * turned[2 * rows : 3 * rows] - csc * turned[3 * rows : 4 * rows]
            weight = jnp.where(order_int > 0, 2.0, 1.0)
            out = []
            for value in (turned[:rows], rotated, slopes):
                value = jnp.where(slot < chunk // 2, value * weight, 0.0)
                swapped = pltpu.roll(value, 2 * SLOTS, 1)
                out.append(
                    jnp.where(
                        odd_row == half,
                        value,
                        jnp.where(
                            odd_row == 1, pltpu.roll(swapped, 1, 0), pltpu.roll(swapped, rows - 1, 0)
                        ),
                    )
                )
            return jnp.concatenate(out, axis=0).astype(BF16)

        if t == 0:
            pl.semaphore_wait(barrier, blocks - 1 + groups - 1)

        def send(k, carry):
            for j in range(4):
                dest = lax.rem(me + 4 * k + j, blocks)
                send_x[t, dest] = message(dest)
            for j in range(4):
                o = 4 * k + j
                dest = lax.rem(me + o, blocks)

                @pl.when(o > 0)
                def _():
                    copy_x(t, dest, me).start()

            return carry

        lax.fori_loop(0, blocks // 4, send, 0)
        recv_x[me, t] = send_x[t, me]

    load_fine.wait()
    load_coarse.wait()

    def fill(n, carry):
        table[n] = (
            fine[0] * coarse[0, pl.ds(n, 1), :] + fine[1] * coarse[1, pl.ds(n, 1), :]
        ).astype(BF16)
        return carry

    lax.fori_loop(0, nblk, fill, 0)

    def whole(ref, count, sem):
        part = ref.at[pl.ds(0, count)]
        return pltpu.make_async_copy(part, part, sem)

    whole(recv_x, blocks - 1, rx).wait()

    pieces = recv_x[...].reshape(nblk, 3 * rows, LANES)
    images = []
    for img in range(4):
        sign = image_signs(img).astype(BF16)
        images.append(
            jnp.concatenate([pieces[n] * sign for n in range(nblk)], axis=1)
        )
    stacked = jnp.concatenate(images, axis=0)
    maps = jnp.dot(
        stacked, table[...].reshape(nblk * LANES, width), preferred_element_type=F32
    )
    flows = []
    for img in range(4):
        base = img * 3 * rows
        product = mask[img] * maps[base : base + rows]
        flows.append(product * maps[base + 2 * rows : base + 3 * rows])
        flows.append(product * maps[base + rows : base + 2 * rows])
    flows = jnp.concatenate(flows, axis=0).astype(BF16)
    for n in range(nblk):
        part = lax.dot_general(flows, table[n], NT, preferred_element_type=F32)
        total = part[: 2 * rows]
        for img in range(1, 4):
            total = total + part[2 * rows * img : 2 * rows * (img + 1)] * image_signs(img)
        send_y[n // chunks, n % chunks] = (total * scale).astype(BF16)

    def copy_y(dest, source):
        return pltpu.make_async_remote_copy(
            src_ref=send_y.at[dest],
            dst_ref=recv_y.at[source],
            send_sem=sy,
            recv_sem=ry.at[source],
            device_id={"blk": dest},
            device_id_type=MESH,
        )

    def put_y(o, carry):
        copy_y(lax.rem(me + o, blocks), me).start()
        return carry

    lax.fori_loop(1, blocks, put_y, 0)
    recv_y[me] = send_y[me]

    def copy_g(o, source, group):
        return pltpu.make_async_remote_copy(
            src_ref=recv_y.at[source],
            dst_ref=gath_y.at[group, source],
            send_sem=sg,
            recv_sem=rg,
            device_id={"sims": lax.rem(mine + o, groups)},
            device_id_type=MESH,
        )

    def spread(source):
        for o in range(1, groups):
            copy_g(o, source, mine).start()

    spread(me)

    def pass_y(o, carry):
        source = lax.rem(me + o, blocks)
        copy_y(source, source).wait_recv()
        spread(source)
        return carry

    lax.fori_loop(1, blocks, pass_y, 0)

    wide = blocks * 2 * rows
    spot = lax.broadcasted_iota(jnp.int32, (rows, wide), 1)
    srow = lax.broadcasted_iota(jnp.int32, (rows, wide), 0)
    same = (spot // 2) % sims == srow % sims
    flow = (spot // rows) % 2
    mask_first = jnp.where(same & (flow == 0), 1.0, 0.0)
    mask_second = jnp.where(same & (flow == 1), jnp.where(srow < sims, 1.0, -1.0), 0.0)
    low_rows = srow < sims
    pick_row = lax.broadcasted_iota(jnp.int32, (wide, quad * cycles), 0)
    pick_col = lax.broadcasted_iota(jnp.int32, (wide, quad * cycles), 1)
    chosen = (pick_row // (2 * rows)) * 2 + pick_row % 2 == pick_col % cycles
    pick = jnp.where(chosen, 1.0, 0.0).astype(BF16)
    member = lax.broadcasted_iota(jnp.int32, (rows, quad * cycles), 1) // cycles
    for t in range(chunks):
        cols[t] = recv_y[:, t].astype(F32).reshape(wide, LANES).T

    def unpack(n, carry):
        t = n // per_chunk
        g = n % per_chunk
        stack = []
        for p in range(2):
            for j in range(quad):
                line = p * SLOTS + quad * g + j
                real = cols[t, pl.ds(line, 1), :]
                imag = cols[t, pl.ds(line + 2 * SLOTS, 1), :]
                stack.append(jnp.where(low_rows, real, imag) * mask_first)
                stack.append(jnp.where(low_rows, imag, real) * mask_second)
        out = jnp.dot(
            jnp.concatenate(stack, axis=0).astype(BF16), pick, preferred_element_type=F32
        )
        for p in range(2):
            pieces = []
            for j in range(quad):
                base = 2 * rows * (p * quad + j)
                one = out[base : base + rows]
                two = out[base + rows : base + 2 * rows]
                tilted = (tilt_row * one).astype(BF16).astype(F32)
                for value in (tilted, one, two):
                    pieces.append(jnp.where(member == j, value, 0.0))
            coefs_y[2 * n + p] = jnp.concatenate(pieces, axis=0).astype(BF16)
        return carry

    lax.fori_loop(0, steps, unpack, 0)

    def legs(n, p):
        return jnp.concatenate(
            [leg[n * GROUP + 2 * j + p] for j in range(quad)], axis=0
        )

    def project(n, carry):
        for p in range(2):
            out = jnp.dot(coefs_y[2 * n + p], legs(n, p), preferred_element_type=F32)
            for j in range(quad):
                base = 3 * rows * j
                order = (first + n * GROUP + 2 * j + p).astype(F32) * (1.0 / degrees)
                est[n * GROUP + 2 * j + p] = (
                    filt[4:5, :] * out[base : base + rows]
                    - lad[2 * n + p, j : j + 1, :]
                    * pltpu.roll(out[base + rows : base + 2 * rows], 1, 1)
                    + order * out[base + 2 * rows : base + 3 * rows]
                )
        return carry

    lax.fori_loop(0, steps, project, 0)

    whole(gath_y, groups - 1, rg).wait()

    def gather_sums(b, carry):
        tilt = jnp.where(
            row8 % 2 == 0, ang[2, pl.ds(2 * b, 1), :], ang[2, pl.ds(2 * b + 1, 1), :]
        )
        for t in range(chunks):
            one = jnp.zeros((rows, LANES), F32)
            two = jnp.zeros((rows, LANES), F32)
            tilted = jnp.zeros((rows, LANES), F32)
            for o in range(groups):
                if o == 0:
                    value = recv_y[b, t].astype(F32)
                else:
                    value = gath_y[lax.rem(mine + o, groups), b, t].astype(F32)
                one = one + value[:rows]
                two = two + value[rows:]
                tilted = tilted + (tilt * value[:rows]).astype(BF16).astype(F32)
            out = []
            for value in (one, two, tilted):
                value = value + pltpu.roll(value, 2, 0)
                out.append(value + pltpu.roll(value, 4, 0))
            parts[b, t] = jnp.concatenate(out + [jnp.zeros_like(one)], axis=0)
        return carry

    lax.fori_loop(0, blocks, gather_sums, 0)
    for t in range(chunks):
        for k in range(2):
            fcols[t, k] = parts[:, t, 2 * rows * k : 2 * rows * (k + 1), :].reshape(wide, LANES).T
    head = (pick_row // 2) % sims == 0
    pick_one = jnp.where(chosen & head & ((pick_row // rows) % 2 == 0), 1.0, 0.0).astype(BF16)
    pick_two = jnp.where(chosen & head & ((pick_row // rows) % 2 == 1), 1.0, 0.0).astype(BF16)
    member_rows = member == lax.broadcasted_iota(jnp.int32, (rows, quad * cycles), 0) % quad

    def split(value):
        upper = value.astype(BF16)
        return [upper, (value - upper.astype(F32)).astype(BF16)]

    def funpack(n, carry):
        t = n // per_chunk
        g = n % per_chunk
        ones = []
        twos = []
        for p in range(2):
            tiles_two = []
            for kind in range(2):
                tile = None
                for c in range(2):
                    for j in range(quad):
                        line = p * SLOTS + quad * g + j + 2 * SLOTS * c
                        row = fcols[t, kind, pl.ds(line, 1), :]
                        tile = row if tile is None else jnp.where(srow == quad * c + j, row, tile)
                tiles_two.append(tile)
            ones += split(tiles_two[1])
            ones += split(tiles_two[0])
            twos += split(
                jnp.where(low_rows, pltpu.roll(tiles_two[0], quad, 0), -pltpu.roll(tiles_two[0], quad, 0))
            )
        out_one = jnp.dot(jnp.concatenate(ones, axis=0), pick_one, preferred_element_type=F32)
        out_two = jnp.dot(jnp.concatenate(twos, axis=0), pick_two, preferred_element_type=F32)
        for p in range(2):
            pieces = [out_one[rows * (4 * p + k) : rows * (4 * p + k + 1)] for k in range(4)]
            pieces += [out_two[rows * (2 * p + k) : rows * (2 * p + k + 1)] for k in range(2)]
            coefs_f[2 * n + p] = jnp.concatenate(
                [jnp.where(member_rows, value, 0.0) for value in pieces], axis=0
            ).astype(BF16)
        return carry

    lax.fori_loop(0, steps, funpack, 0)

    share = degrees // groups
    every = 1.0 / (sims * groups)

    def project_field(n, carry):
        for p in range(2):
            out = jnp.dot(coefs_f[2 * n + p], legs(n, p), preferred_element_type=F32)
            one, two, three = [
                out[2 * rows * k : 2 * rows * k + rows] + out[2 * rows * k + rows : 2 * rows * (k + 1)]
                for k in range(3)
            ]
            whole = (
                filt[4:5, :] * one
                - lad[2 * n + p] * pltpu.roll(two, 1, 1)
                + (quad_orders(n, p) * (1.0 / degrees)) * three
            )
            field[2 * n + p] = whole * every
            part = whole[:, 0:share]
            for g in range(1, groups):
                part = jnp.where(mine == g, whole[:, g * share : (g + 1) * share], part)
            for j in range(quad):
                for c in range(2):
                    field_out[n * GROUP + 2 * j + p, c : c + 1, :] = part[
                        quad * c + j : quad * c + j + 1
                    ]
        return carry

    lax.fori_loop(0, steps, project_field, 0)

    def copy_s(k, dest, source):
        part = pl.ds(k * share, share)
        return pltpu.make_async_remote_copy(
            src_ref=box.at[blocks, :, part],
            dst_ref=box.at[source, :, part],
            send_sem=ss,
            recv_sem=rs,
            device_id={"blk": dest},
            device_id_type=MESH,
        )

    share_row = lax.broadcasted_iota(jnp.int32, (rows, share), 0)
    for k in range(groups):
        here = slice(k * share, (k + 1) * share)

        def power(n, carry):
            auto, cross = carry
            for p in range(2):
                for j in range(quad):
                    weight = jnp.where(first + n * GROUP + 2 * j + p > 0, 2.0, 1.0)
                    mean = jnp.where(
                        share_row < sims,
                        field[2 * n + p, j : j + 1, here],
                        field[2 * n + p, quad + j : quad + j + 1, here],
                    )
                    residual = est[n * GROUP + 2 * j + p, :, here] - mean
                    weighted = weight * residual
                    auto = auto + weighted * residual
                    cross = cross + weighted * pltpu.roll(residual, rows - 1, 0)
            return auto, cross

        zero = jnp.zeros((rows, share), F32)
        auto, cross = lax.fori_loop(0, steps, power, (zero, zero))
        auto = auto + pltpu.roll(auto, sims, 0)
        cross = cross + pltpu.roll(cross, sims, 0)
        cross = jnp.where(share_row % 2 == 0, cross, pltpu.roll(cross, 1, 0))
        box[blocks, :, here] = jnp.where(share_row < sims, auto, cross) * filt[5:6, here]

        def put_s(o, carry):
            copy_s(k, lax.rem(me + o, blocks), me).start()
            return carry

        lax.fori_loop(1, blocks, put_s, 0)

    box[me] = box[blocks]
    whole(box, blocks - 1, rs).wait()

    def add_s(b, value):
        return value + box[b]

    result = lax.fori_loop(0, blocks, add_s, jnp.zeros((rows, degrees), F32))
    spec_out[...] = result

    whole(recv_x, blocks - 1, sx).wait()
    whole(recv_y, blocks - 1, sy).wait()
    whole(gath_y, groups - 1, sg).wait()
    whole(box, blocks - 1, ss).wait()


def angle_tables(blocks, chunks, chunk, pixels, width):
    pixel = np.arange(width)

    def waves(orders):
        turn = 2.0 * np.pi / pixels * ((orders[:, None] * pixel[None, :]) % pixels)
        return np.cos(turn), np.sin(turn)

    even = waves(2 * np.arange(SLOTS))
    odd = waves(2 * np.arange(SLOTS) + 1)
    fine = np.stack(
        [
            np.concatenate([even[0], odd[0], -even[1], -odd[1]]),
            np.concatenate([-even[1], -odd[1], -even[0], -odd[0]]),
        ]
    )
    coarse = np.stack(waves(chunk * np.arange(blocks * chunks)))
    return fine.astype(np.float32), coarse.astype(np.float32)


def per_device(sim_alm, t_filter, wiener_filter, colatitude, legendre, pixel_mask):
    orders, sims, parts, degrees = sim_alm.shape
    cycles = legendre.shape[2]
    pixels = pixel_mask.shape[1]
    blocks = lax.axis_size("blk")
    groups = lax.axis_size("sims")
    rows = sims * parts
    tiles = degrees // LANES
    assert rows == 8 and cycles == 2 * blocks and blocks % 4 == 0
    chunk = chunk_of(orders)
    chunks = orders // chunk
    nblk = blocks * chunks
    width = pixels // 4 + LANES
    steps = orders // GROUP
    quads = 2 * steps
    wide = blocks * 2 * rows

    fine, coarse = angle_tables(blocks, chunks, chunk, pixels, width)
    leg_rows = jnp.transpose(legendre, (0, 2, 1))
    alm_tiles = jnp.transpose(
        sim_alm.reshape(orders, sims, parts, tiles, LANES), (0, 1, 3, 2, 4)
    )

    hbm = pl.BlockSpec(memory_space=pl.ANY)
    vmem = pl.BlockSpec(memory_space=pltpu.VMEM)
    dma = pltpu.SemaphoreType.DMA
    field, spectra = pl.pallas_call(
        functools.partial(kernel, chunk=chunk, scale=2.0 * math.pi / pixels, pixels=pixels),
        in_specs=[hbm, hbm, hbm, hbm, vmem, vmem, vmem, vmem],
        out_specs=[vmem, vmem],
        out_shape=[
            jax.ShapeDtypeStruct((orders, 2, degrees // groups), F32),
            jax.ShapeDtypeStruct((rows, degrees), F32),
        ],
        scratch_shapes=[
            pltpu.VMEM((orders, tiles, rows, LANES), BF16),
            pltpu.VMEM((orders, cycles, degrees), BF16),
            pltpu.VMEM((2, LANES, width), F32),
            pltpu.VMEM((2, nblk, width), F32),
            pltpu.VMEM((8, degrees), F32),
            pltpu.VMEM((3, cycles, LANES), F32),
            pltpu.VMEM((4, rows, width), F32),
            pltpu.VMEM((quads, rows, degrees), F32),
            pltpu.VMEM((2, rows, degrees), F32),
            pltpu.VMEM((2 * SLOTS * cycles, LANES), F32),
            pltpu.VMEM((chunks, blocks, 3 * rows, LANES), BF16),
            pltpu.VMEM((blocks, chunks, 3 * rows, LANES), BF16),
            pltpu.VMEM((nblk, LANES, width), BF16),
            pltpu.VMEM((blocks, chunks, 2 * rows, LANES), BF16),
            pltpu.VMEM((blocks, chunks, 2 * rows, LANES), BF16),
            pltpu.VMEM((groups, blocks, chunks, 2 * rows, LANES), BF16),
            pltpu.VMEM((chunks, LANES, wide), F32),
            pltpu.VMEM((chunks, 2, LANES, wide), F32),
            pltpu.VMEM((blocks, chunks, 4 * rows, LANES), F32),
            pltpu.VMEM((quads, 12 * rows, 4 * cycles), BF16),
            pltpu.VMEM((quads, 6 * rows, 4 * cycles), BF16),
            pltpu.VMEM((orders, rows, degrees), F32),
            pltpu.VMEM((quads, rows, degrees), F32),
            pltpu.VMEM((1 + blocks, rows, degrees), F32),
            dma((DEPTH, 2)),
            dma((2,)),
            dma,
            dma,
            dma,
            dma((blocks,)),
            dma,
            dma,
            dma,
            dma,
        ],
        compiler_params=pltpu.CompilerParams(
            collective_id=0, has_side_effects=True, vmem_limit_bytes=VMEM_LIMIT
        ),
        name="lensing",
    )(
        alm_tiles, leg_rows, jnp.asarray(fine), jnp.asarray(coarse),
        t_filter, wiener_filter, colatitude, pixel_mask,
    )

    return (field, jnp.transpose(spectra.reshape(2, sims, degrees), (1, 0, 2)))


def solution(mesh):
    placed = (P("blk", "sims", None, None), P(), P(), P(), P("blk", None, None), P("blk", None))
    return jax.shard_map(
        per_device,
        mesh=mesh,
        in_specs=placed,
        out_specs=(P("blk", None, "sims"), P("sims", None, None)),
        check_vma=False,
    )
```

```python
import functools
import math

import jax
import jax.numpy as jnp
import numpy as np
from jax import lax
from jax.experimental import pallas as pl
from jax.experimental.pallas import tpu as pltpu
from jax.sharding import PartitionSpec as P

F32 = jnp.float32
BF16 = jnp.bfloat16
LANES = 128
SLOTS = 32
GROUP = 8
DEPTH = 6
VMEM_LIMIT = 54 * 1024 * 1024
MESH = pl.DeviceIdType.MESH
NT = (((1,), (1,)), ((), ()))
SIGNS = ((1, 1, 1, 1), (1, -1, -1, 1), (1, -1, 1, -1), (1, 1, -1, -1))


def chunk_of(orders):
    best = 0
    for size in range(GROUP, 2 * SLOTS + 1, GROUP):
        if orders % size == 0:
            best = size
    assert best > 0
    return best


def repeat(count, together, body):
    def several(i, carry):
        for k in range(together):
            body(i * together + k)
        return carry

    lax.fori_loop(0, count // together, several, 0)


def image_signs(img):
    part = lax.broadcasted_iota(jnp.int32, (1, LANES), 1) // SLOTS
    sign = jnp.ones((1, LANES), F32)
    for k in range(4):
        if SIGNS[img][k] < 0:
            sign = jnp.where(part == k, -1.0, sign)
    return sign


def kernel(
    alm_hbm, leg_hbm, fine_hbm, coarse_hbm, t_filter, w_filter, colatitude, seen,
    field_out, spec_out,
    alm, leg, fine, coarse, filt, ang, mask, lad, raised_rows, sums, send_x, recv_x, table,
    send_y, recv_y, gath_y, cols, fcols, parts, coefs_y, coefs_f, est, field, box,
    sem_in, sem_c, sx, rx, sy, ry, sg, rg, ss, rs,
    *, chunk, scale, pixels,
):
    orders, tiles = alm.shape[:2]
    rows = alm.shape[2]
    sims = rows // 2
    degrees = tiles * LANES
    cycles = leg.shape[1]
    blocks = recv_y.shape[0]
    chunks = recv_y.shape[1]
    groups = gath_y.shape[0]
    steps = orders // GROUP
    per_chunk = chunk // GROUP
    nblk = blocks * chunks
    width = table.shape[2]
    quad = GROUP // 2
    joint = 2 if per_chunk % 2 == 0 else 1
    me = lax.axis_index("blk")
    mine = lax.axis_index("sims")
    first = me * orders

    barrier = pltpu.get_barrier_semaphore()

    def greet_blk(o, carry):
        pl.semaphore_signal(
            barrier, inc=1, device_id={"blk": lax.rem(me + o, blocks)}, device_id_type=MESH
        )
        return carry

    def greet_sims(o, carry):
        pl.semaphore_signal(
            barrier, inc=1, device_id={"sims": lax.rem(mine + o, groups)}, device_id_type=MESH
        )
        return carry

    def start_load(n):
        part = pl.ds(n * GROUP, GROUP)
        pltpu.make_async_copy(leg_hbm.at[part], leg.at[part], sem_in.at[n % DEPTH, 0]).start()
        for s in range(sims):
            pltpu.make_async_copy(
                alm_hbm.at[part, s],
                alm.at[part, :, pl.ds(2 * s, 2), :],
                sem_in.at[n % DEPTH, 1],
            ).start()

    def wait_load(n):
        part = pl.ds(n * GROUP, GROUP)
        pltpu.make_async_copy(leg.at[part], leg.at[part], sem_in.at[n % DEPTH, 0]).wait()
        pltpu.make_async_copy(alm.at[part], alm.at[part], sem_in.at[n % DEPTH, 1]).wait()

    load_fine = pltpu.make_async_copy(fine_hbm, fine, sem_c.at[0])
    load_coarse = pltpu.make_async_copy(coarse_hbm, coarse, sem_c.at[1])

    ahead = min(DEPTH, steps)
    for n in range(ahead):
        start_load(n)
    load_fine.start()
    load_coarse.start()
    lax.fori_loop(1, blocks, greet_blk, 0)
    lax.fori_loop(1, groups, greet_sims, 0)

    degree = lax.broadcasted_iota(jnp.int32, (1, degrees), 1).astype(F32)
    lane = lax.broadcasted_iota(jnp.int32, (1, LANES), 1)
    slot = lane % SLOTS
    parity = (lane // SLOTS) % 2
    half = lane // (2 * SLOTS)
    row8 = lax.broadcasted_iota(jnp.int32, (rows, LANES), 0)
    column = lax.broadcasted_iota(jnp.int32, (rows, 1), 0)

    t_row = t_filter[...].reshape(1, degrees)
    w_row = w_filter[...].reshape(1, degrees)
    filt[0] = jnp.broadcast_to(t_row, (rows, degrees))
    filt[1] = jnp.broadcast_to(w_row, (rows, degrees))
    filt[2] = jnp.broadcast_to(degree * w_row, (rows, degrees))
    filt[3] = jnp.broadcast_to((2.0 * degree + 1.0) / jnp.maximum(2.0 * degree - 1.0, 1.0), (rows, degrees))
    filt[4] = jnp.broadcast_to(degree * (1.0 / degrees), (rows, degrees))
    filt[5] = jnp.broadcast_to(1.0 / (2.0 * degree + 1.0), (rows, degrees))

    angle = colatitude[...].reshape(1, cycles)
    cosine = jnp.cos(angle)
    cosecant = 1.0 / jnp.sin(angle)
    square_row = lax.broadcasted_iota(jnp.int32, (cycles, cycles), 0)
    square_col = lax.broadcasted_iota(jnp.int32, (cycles, cycles), 1)
    for k, value in enumerate((cosine * cosecant, cosecant, cosine)):
        spread_out = jnp.where(square_row == square_col, value, 0.0)
        ang[k] = jnp.broadcast_to(
            jnp.sum(spread_out, axis=1, keepdims=True), (cycles, LANES)
        )
    tilt_row = jnp.concatenate([cosine] * quad, axis=1)

    quarter = pixels // 4
    both = seen[...].astype(F32)
    both = jnp.where(
        lax.broadcasted_iota(jnp.int32, (rows, pixels), 0) % 2 == 0, both[0:1], both[1:2]
    )
    both = jnp.concatenate([both, jnp.zeros((rows, LANES), F32)], axis=1)
    turn_row = lax.broadcasted_iota(jnp.int32, (2 * LANES, LANES), 0)
    turn_col = lax.broadcasted_iota(jnp.int32, (2 * LANES, LANES), 1)
    turn = jnp.where(turn_row + turn_col == LANES, 1.0, 0.0).astype(BF16)
    half_seen = both.astype(BF16)
    for n in range(width // LANES):
        pixel = lane + n * LANES
        here = slice(n * LANES, (n + 1) * LANES)
        back = pixels // 2 - (n + 1) * LANES
        straight = both[:, n * LANES : (n + 1) * LANES]
        mask[0, :, here] = jnp.where(pixel <= quarter, straight, 0.0)
        mirror = jnp.dot(
            half_seen[:, back : back + 2 * LANES], turn, preferred_element_type=F32
        )
        mask[1, :, here] = jnp.where(pixel < quarter, mirror, 0.0)
        at = pixels // 2 + n * LANES
        mask[2, :, here] = jnp.where(
            (pixel > 0) & (pixel <= quarter), both[:, at : at + LANES], 0.0
        )
        back = pixels - (n + 1) * LANES
        mirror = jnp.dot(
            half_seen[:, back : back + 2 * LANES], turn, preferred_element_type=F32
        )
        mask[3, :, here] = jnp.where((pixel > 0) & (pixel < quarter), mirror, 0.0)

    def quad_orders(n, p):
        return (first + n * GROUP + 2 * (column % quad) + p).astype(F32)

    def copy_x(t, dest, source):
        return pltpu.make_async_remote_copy(
            src_ref=send_x.at[t, dest],
            dst_ref=recv_x.at[source, t],
            send_sem=sx,
            recv_sem=rx,
            device_id={"blk": dest},
            device_id_type=MESH,
        )

    for t in range(chunks):

        def block_sums(i, k):
            n = t * per_chunk + i
            for p in range(2):
                order = quad_orders(n, p)
                square = (degree * degree - order * order) * filt[3]
                ladder = jnp.where(
                    degree > order, square * lax.rsqrt(jnp.maximum(square, 1.0)), 0.0
                )
                lad[2 * n + p] = ladder * (1.0 / degrees)
                raised_rows[2 * k + p] = ladder * filt[1]
            for u in range(GROUP):
                values = jnp.concatenate(
                    [alm[n * GROUP + u, k].astype(F32) for k in range(tiles)], axis=1
                )
                raised = raised_rows[2 * k + u % 2, pl.ds(u // 2, rows, stride=0), :] * values
                lowered = pltpu.roll(raised, degrees - 1, 1)
                coefs = jnp.concatenate(
                    [filt[0] * values, filt[1] * values, filt[2] * values, lowered],
                    axis=0,
                ).astype(BF16)
                sums[pl.ds((i * GROUP + u) * cycles, cycles), 0 : 4 * rows] = lax.dot_general(
                    leg[n * GROUP + u], coefs, NT, preferred_element_type=F32
                )

        def step(i, carry):
            for k in range(joint):
                n = t * per_chunk + i * joint + k
                wait_load(n)

                @pl.when(n + ahead < steps)
                def _():
                    start_load(n + ahead)

            for k in range(joint):
                block_sums(i * joint + k, k)
            return carry

        lax.fori_loop(0, per_chunk // joint, step, 0)

        def message(dest):
            pieces = []
            for r in range(2):
                for p in range(2):
                    pieces.append(
                        sums[pl.ds(p * cycles + 2 * dest + r, SLOTS, stride=2 * cycles), :]
                    )
            turned = jnp.concatenate(pieces, axis=0).T
            order_int = first + t * chunk + 2 * slot + parity
            order = order_int.astype(F32)
            cot = jnp.where(
                half == 0, ang[0, pl.ds(2 * dest, 1), :], ang[0, pl.ds(2 * dest + 1, 1), :]
            )
            csc = jnp.where(
                half == 0, ang[1, pl.ds(2 * dest, 1), :], ang[1, pl.ds(2 * dest + 1, 1), :]
            )
            wave = turned[rows : 2 * rows]
            odd_row = row8 % 2
            rotated = jnp.where(
                odd_row == 0, -pltpu.roll(wave, rows - 1, 0), pltpu.roll(wave, 1, 0)
            ) * (csc * order)
            slopes = cot * turned[2 * rows : 3 * rows] - csc * turned[3 * rows : 4 * rows]
            weight = jnp.where(order_int > 0, 2.0, 1.0)
            out = []
            for value in (turned[:rows], rotated, slopes):
                value = jnp.where(slot < chunk // 2, value * weight, 0.0)
                swapped = pltpu.roll(value, 2 * SLOTS, 1)
                out.append(
                    jnp.where(
                        odd_row == half,
                        value,
                        jnp.where(
                            odd_row == 1, pltpu.roll(swapped, 1, 0), pltpu.roll(swapped, rows - 1, 0)
                        ),
                    )
                )
            return jnp.concatenate(out, axis=0).astype(BF16)

        if t == 0:
            pl.semaphore_wait(barrier, blocks - 1 + groups - 1)

        def send(k, carry):
            for j in range(4):
                dest = lax.rem(me + 4 * k + j, blocks)
                send_x[t, dest] = message(dest)
            for j in range(4):
                o = 4 * k + j
                dest = lax.rem(me + o, blocks)

                @pl.when(o > 0)
                def _():
                    copy_x(t, dest, me).start()

            return carry

        lax.fori_loop(0, blocks // 4, send, 0)
        recv_x[me, t] = send_x[t, me]

    load_fine.wait()
    load_coarse.wait()

    def fill(n, carry):
        table[n] = (
            fine[0] * coarse[0, pl.ds(n, 1), :] + fine[1] * coarse[1, pl.ds(n, 1), :]
        ).astype(BF16)
        return carry

    lax.fori_loop(0, nblk, fill, 0)

    def whole(ref, count, sem):
        part = ref.at[pl.ds(0, count)]
        return pltpu.make_async_copy(part, part, sem)

    whole(recv_x, blocks - 1, rx).wait()

    pieces = recv_x[...].reshape(nblk, 3 * rows, LANES)
    images = []
    for img in range(4):
        sign = image_signs(img).astype(BF16)
        images.append(
            jnp.concatenate([pieces[n] * sign for n in range(nblk)], axis=1)
        )
    stacked = jnp.concatenate(images, axis=0)
    maps = jnp.dot(
        stacked, table[...].reshape(nblk * LANES, width), preferred_element_type=F32
    )
    flows = []
    for img in range(4):
        base = img * 3 * rows
        product = mask[img] * maps[base : base + rows]
        flows.append(product * maps[base + 2 * rows : base + 3 * rows])
        flows.append(product * maps[base + rows : base + 2 * rows])
    flows = jnp.concatenate(flows, axis=0).astype(BF16)
    for n in range(nblk):
        part = lax.dot_general(flows, table[n], NT, preferred_element_type=F32)
        total = part[: 2 * rows]
        for img in range(1, 4):
            total = total + part[2 * rows * img : 2 * rows * (img + 1)] * image_signs(img)
        send_y[n // chunks, n % chunks] = (total * scale).astype(BF16)

    def copy_y(dest, source):
        return pltpu.make_async_remote_copy(
            src_ref=send_y.at[dest],
            dst_ref=recv_y.at[source],
            send_sem=sy,
            recv_sem=ry.at[source],
            device_id={"blk": dest},
            device_id_type=MESH,
        )

    def put_y(o, carry):
        copy_y(lax.rem(me + o, blocks), me).start()
        return carry

    lax.fori_loop(1, blocks, put_y, 0)
    recv_y[me] = send_y[me]

    def copy_g(o, source, group):
        return pltpu.make_async_remote_copy(
            src_ref=recv_y.at[source],
            dst_ref=gath_y.at[group, source],
            send_sem=sg,
            recv_sem=rg,
            device_id={"sims": lax.rem(mine + o, groups)},
            device_id_type=MESH,
        )

    def spread(source):
        for o in range(1, groups):
            copy_g(o, source, mine).start()

    spread(me)

    def pass_y(o, carry):
        source = lax.rem(me + o, blocks)
        copy_y(source, source).wait_recv()
        spread(source)
        return carry

    lax.fori_loop(1, blocks, pass_y, 0)

    wide = blocks * 2 * rows
    spot = lax.broadcasted_iota(jnp.int32, (rows, wide), 1)
    srow = lax.broadcasted_iota(jnp.int32, (rows, wide), 0)
    same = (spot // 2) % sims == srow % sims
    flow = (spot // rows) % 2
    mask_first = jnp.where(same & (flow == 0), 1.0, 0.0)
    mask_second = jnp.where(same & (flow == 1), jnp.where(srow < sims, 1.0, -1.0), 0.0)
    low_rows = srow < sims
    pick_row = lax.broadcasted_iota(jnp.int32, (wide, quad * cycles), 0)
    pick_col = lax.broadcasted_iota(jnp.int32, (wide, quad * cycles), 1)
    chosen = (pick_row // (2 * rows)) * 2 + pick_row % 2 == pick_col % cycles
    pick = jnp.where(chosen, 1.0, 0.0).astype(BF16)
    member = lax.broadcasted_iota(jnp.int32, (rows, quad * cycles), 1) // cycles
    for t in range(chunks):
        cols[t] = recv_y[:, t].astype(F32).reshape(wide, LANES).T

    def unpack(n):
        t = n // per_chunk
        g = n % per_chunk
        stack = []
        for p in range(2):
            for j in range(quad):
                line = p * SLOTS + quad * g + j
                real = cols[t, pl.ds(line, 1), :]
                imag = cols[t, pl.ds(line + 2 * SLOTS, 1), :]
                stack.append(jnp.where(low_rows, real, imag) * mask_first)
                stack.append(jnp.where(low_rows, imag, real) * mask_second)
        out = jnp.dot(
            jnp.concatenate(stack, axis=0).astype(BF16), pick, preferred_element_type=F32
        )
        for p in range(2):
            pieces = []
            for j in range(quad):
                base = 2 * rows * (p * quad + j)
                one = out[base : base + rows]
                two = out[base + rows : base + 2 * rows]
                tilted = (tilt_row * one).astype(BF16).astype(F32)
                for value in (tilted, one, two):
                    pieces.append(jnp.where(member == j, value, 0.0))
            coefs_y[2 * n + p] = jnp.concatenate(pieces, axis=0).astype(BF16)

    repeat(steps, joint, unpack)

    def legs(n, p):
        return jnp.concatenate(
            [leg[n * GROUP + 2 * j + p] for j in range(quad)], axis=0
        )

    def project(n):
        for p in range(2):
            out = jnp.dot(coefs_y[2 * n + p], legs(n, p), preferred_element_type=F32)
            for j in range(quad):
                base = 3 * rows * j
                order = (first + n * GROUP + 2 * j + p).astype(F32) * (1.0 / degrees)
                est[n * GROUP + 2 * j + p] = (
                    filt[4] * out[base : base + rows]
                    - lad[2 * n + p, pl.ds(j, rows, stride=0), :]
                    * pltpu.roll(out[base + rows : base + 2 * rows], 1, 1)
                    + order * out[base + 2 * rows : base + 3 * rows]
                )

    repeat(steps, joint, project)

    whole(gath_y, groups - 1, rg).wait()

    def gather_sums(b, carry):
        tilt = jnp.where(
            row8 % 2 == 0, ang[2, pl.ds(2 * b, 1), :], ang[2, pl.ds(2 * b + 1, 1), :]
        )
        for t in range(chunks):
            one = jnp.zeros((rows, LANES), F32)
            two = jnp.zeros((rows, LANES), F32)
            tilted = jnp.zeros((rows, LANES), F32)
            for o in range(groups):
                if o == 0:
                    value = recv_y[b, t].astype(F32)
                else:
                    value = gath_y[lax.rem(mine + o, groups), b, t].astype(F32)
                one = one + value[:rows]
                two = two + value[rows:]
                tilted = tilted + (tilt * value[:rows]).astype(BF16).astype(F32)
            out = []
            for value in (one, two, tilted):
                value = value + pltpu.roll(value, 2, 0)
                out.append(value + pltpu.roll(value, 4, 0))
            parts[b, t] = jnp.concatenate(out + [jnp.zeros_like(one)], axis=0)
        return carry

    lax.fori_loop(0, blocks, gather_sums, 0)
    for t in range(chunks):
        for k in range(2):
            fcols[t, k] = parts[:, t, 2 * rows * k : 2 * rows * (k + 1), :].reshape(wide, LANES).T
    head = (pick_row // 2) % sims == 0
    pick_one = jnp.where(chosen & head & ((pick_row // rows) % 2 == 0), 1.0, 0.0).astype(BF16)
    pick_two = jnp.where(chosen & head & ((pick_row // rows) % 2 == 1), 1.0, 0.0).astype(BF16)
    member_rows = member == lax.broadcasted_iota(jnp.int32, (rows, quad * cycles), 0) % quad

    def split(value):
        upper = value.astype(BF16)
        return [upper, (value - upper.astype(F32)).astype(BF16)]

    def funpack(n):
        t = n // per_chunk
        g = n % per_chunk
        ones = []
        twos = []
        for p in range(2):
            tiles_two = []
            for kind in range(2):
                tile = None
                for c in range(2):
                    for j in range(quad):
                        line = p * SLOTS + quad * g + j + 2 * SLOTS * c
                        row = fcols[t, kind, pl.ds(line, 1), :]
                        tile = row if tile is None else jnp.where(srow == quad * c + j, row, tile)
                tiles_two.append(tile)
            ones += split(tiles_two[1])
            ones += split(tiles_two[0])
            twos += split(
                jnp.where(low_rows, pltpu.roll(tiles_two[0], quad, 0), -pltpu.roll(tiles_two[0], quad, 0))
            )
        out_one = jnp.dot(jnp.concatenate(ones, axis=0), pick_one, preferred_element_type=F32)
        out_two = jnp.dot(jnp.concatenate(twos, axis=0), pick_two, preferred_element_type=F32)
        for p in range(2):
            pieces = [out_one[rows * (4 * p + k) : rows * (4 * p + k + 1)] for k in range(4)]
            pieces += [out_two[rows * (2 * p + k) : rows * (2 * p + k + 1)] for k in range(2)]
            coefs_f[2 * n + p] = jnp.concatenate(
                [jnp.where(member_rows, value, 0.0) for value in pieces], axis=0
            ).astype(BF16)

    repeat(steps, joint, funpack)

    share = degrees // groups
    every = 1.0 / (sims * groups)

    def project_field(n):
        for p in range(2):
            out = jnp.dot(coefs_f[2 * n + p], legs(n, p), preferred_element_type=F32)
            one, two, three = [
                out[2 * rows * k : 2 * rows * k + rows] + out[2 * rows * k + rows : 2 * rows * (k + 1)]
                for k in range(3)
            ]
            whole = (
                filt[4] * one
                - lad[2 * n + p] * pltpu.roll(two, 1, 1)
                + (quad_orders(n, p) * (1.0 / degrees)) * three
            )
            for g in range(groups):
                field[g, 2 * n + p] = whole[:, g * share : (g + 1) * share] * every
            part = whole[:, 0:share]
            for g in range(1, groups):
                part = jnp.where(mine == g, whole[:, g * share : (g + 1) * share], part)
            for j in range(quad):
                for c in range(2):
                    field_out[n * GROUP + 2 * j + p, c : c + 1, :] = part[
                        quad * c + j : quad * c + j + 1
                    ]

    repeat(steps, joint, project_field)

    def copy_s(k, dest, source):
        part = pl.ds(k * share, share)
        return pltpu.make_async_remote_copy(
            src_ref=box.at[blocks, :, part],
            dst_ref=box.at[source, :, part],
            send_sem=ss,
            recv_sem=rs,
            device_id={"blk": dest},
            device_id_type=MESH,
        )

    share_row = lax.broadcasted_iota(jnp.int32, (rows, share), 0)
    for k in range(groups):
        here = slice(k * share, (k + 1) * share)

        def power(n, carry):
            auto, cross = carry
            for p in range(2):
                for j in range(quad):
                    mean = jnp.where(
                        share_row < sims,
                        field[k, 2 * n + p, pl.ds(j, rows, stride=0), :],
                        field[k, 2 * n + p, pl.ds(quad + j, rows, stride=0), :],
                    )
                    residual = est[n * GROUP + 2 * j + p, :, here] - mean
                    auto = auto + residual * residual
                    cross = cross + residual * pltpu.roll(residual, rows - 1, 0)
            return auto, cross

        zero = jnp.zeros((rows, share), F32)
        auto, cross = lax.fori_loop(0, steps, power, (zero, zero))
        residual = est[0, :, here] - jnp.where(
            share_row < sims, field[k, 0, 0:1, :], field[k, 0, quad : quad + 1, :]
        )
        residual = jnp.where(me == 0, residual, 0.0)
        auto = 2.0 * auto - residual * residual
        cross = 2.0 * cross - residual * pltpu.roll(residual, rows - 1, 0)
        auto = auto + pltpu.roll(auto, sims, 0)
        cross = cross + pltpu.roll(cross, sims, 0)
        cross = jnp.where(share_row % 2 == 0, cross, pltpu.roll(cross, 1, 0))
        box[blocks, :, here] = jnp.where(share_row < sims, auto, cross) * filt[5, :, here]

        def put_s(o, carry):
            copy_s(k, lax.rem(me + o, blocks), me).start()
            return carry

        lax.fori_loop(1, blocks, put_s, 0)

    box[me] = box[blocks]
    whole(box, blocks - 1, rs).wait()

    def add_s(b, value):
        return value + box[b]

    result = lax.fori_loop(0, blocks, add_s, jnp.zeros((rows, degrees), F32))
    for s in range(sims):
        spec_out[s] = jnp.concatenate([result[s : s + 1], result[sims + s : sims + s + 1]], axis=0)

    whole(recv_x, blocks - 1, sx).wait()
    whole(recv_y, blocks - 1, sy).wait()
    whole(gath_y, groups - 1, sg).wait()
    whole(box, blocks - 1, ss).wait()


def angle_tables(blocks, chunks, chunk, pixels, width):
    pixel = np.arange(width)

    def waves(orders):
        turn = 2.0 * np.pi / pixels * ((orders[:, None] * pixel[None, :]) % pixels)
        return np.cos(turn), np.sin(turn)

    even = waves(2 * np.arange(SLOTS))
    odd = waves(2 * np.arange(SLOTS) + 1)
    fine = np.stack(
        [
            np.concatenate([even[0], odd[0], -even[1], -odd[1]]),
            np.concatenate([-even[1], -odd[1], -even[0], -odd[0]]),
        ]
    )
    coarse = np.stack(waves(chunk * np.arange(blocks * chunks)))
    return fine.astype(np.float32), coarse.astype(np.float32)


def per_device(sim_alm, t_filter, wiener_filter, colatitude, legendre, pixel_mask):
    orders, sims, parts, degrees = sim_alm.shape
    cycles = legendre.shape[2]
    pixels = pixel_mask.shape[1]
    blocks = lax.axis_size("blk")
    groups = lax.axis_size("sims")
    rows = sims * parts
    tiles = degrees // LANES
    assert rows == 8 and cycles == 2 * blocks and blocks % 4 == 0
    chunk = chunk_of(orders)
    chunks = orders // chunk
    nblk = blocks * chunks
    width = pixels // 4 + LANES
    steps = orders // GROUP
    quads = 2 * steps
    wide = blocks * 2 * rows

    fine, coarse = angle_tables(blocks, chunks, chunk, pixels, width)
    leg_rows = jnp.transpose(legendre, (0, 2, 1))
    alm_tiles = jnp.transpose(
        sim_alm.reshape(orders, sims, parts, tiles, LANES), (0, 1, 3, 2, 4)
    )

    hbm = pl.BlockSpec(memory_space=pl.ANY)
    vmem = pl.BlockSpec(memory_space=pltpu.VMEM)
    dma = pltpu.SemaphoreType.DMA
    field, spectra = pl.pallas_call(
        functools.partial(kernel, chunk=chunk, scale=2.0 * math.pi / pixels, pixels=pixels),
        in_specs=[hbm, hbm, hbm, hbm, vmem, vmem, vmem, vmem],
        out_specs=[vmem, vmem],
        out_shape=[
            pltpu.VMEM((orders, 2, degrees // groups), F32),
            pltpu.VMEM((sims, 2, degrees), F32),
        ],
        scratch_shapes=[
            pltpu.VMEM((orders, tiles, rows, LANES), BF16),
            pltpu.VMEM((orders, cycles, degrees), BF16),
            pltpu.VMEM((2, LANES, width), F32),
            pltpu.VMEM((2, nblk, width), F32),
            pltpu.VMEM((6, rows, degrees), F32),
            pltpu.VMEM((3, cycles, LANES), F32),
            pltpu.VMEM((4, rows, width), F32),
            pltpu.VMEM((quads, rows, degrees), F32),
            pltpu.VMEM((4, rows, degrees), F32),
            pltpu.VMEM((2 * SLOTS * cycles, LANES), F32),
            pltpu.VMEM((chunks, blocks, 3 * rows, LANES), BF16),
            pltpu.VMEM((blocks, chunks, 3 * rows, LANES), BF16),
            pltpu.VMEM((nblk, LANES, width), BF16),
            pltpu.VMEM((blocks, chunks, 2 * rows, LANES), BF16),
            pltpu.VMEM((blocks, chunks, 2 * rows, LANES), BF16),
            pltpu.VMEM((groups, blocks, chunks, 2 * rows, LANES), BF16),
            pltpu.VMEM((chunks, LANES, wide), F32),
            pltpu.VMEM((chunks, 2, LANES, wide), F32),
            pltpu.VMEM((blocks, chunks, 4 * rows, LANES), F32),
            pltpu.VMEM((quads, 12 * rows, 4 * cycles), BF16),
            pltpu.VMEM((quads, 6 * rows, 4 * cycles), BF16),
            pltpu.VMEM((orders, rows, degrees), F32),
            pltpu.VMEM((groups, quads, rows, degrees // groups), F32),
            pltpu.VMEM((1 + blocks, rows, degrees), F32),
            dma((DEPTH, 2)),
            dma((2,)),
            dma,
            dma,
            dma,
            dma((blocks,)),
            dma,
            dma,
            dma,
            dma,
        ],
        compiler_params=pltpu.CompilerParams(
            collective_id=0, has_side_effects=True, vmem_limit_bytes=VMEM_LIMIT
        ),
        name="lensing",
    )(
        alm_tiles, leg_rows, jnp.asarray(fine), jnp.asarray(coarse),
        t_filter, wiener_filter, colatitude, pixel_mask,
    )

    return field, spectra


def solution(mesh):
    placed = (P("blk", "sims", None, None), P(), P(), P(), P("blk", None, None), P("blk", None))
    return jax.shard_map(
        per_device,
        mesh=mesh,
        in_specs=placed,
        out_specs=(P("blk", None, "sims"), P("sims", None, None)),
        check_vma=False,
    )
```

```python
import functools
import math

import jax
import jax.numpy as jnp
import numpy as np
from jax import lax
from jax.experimental import pallas as pl
from jax.experimental.pallas import tpu as pltpu
from jax.sharding import PartitionSpec as P

F32 = jnp.float32
BF16 = jnp.bfloat16
LANES = 128
SLOTS = 32
GROUP = 8
DEPTH = 6
HALVES = 2
VMEM_LIMIT = 54 * 1024 * 1024
MESH = pl.DeviceIdType.MESH
NT = (((1,), (1,)), ((), ()))
SIGNS = ((1, 1, 1, 1), (1, -1, -1, 1), (1, -1, 1, -1), (1, 1, -1, -1))


def chunk_of(orders):
    best = 0
    for size in range(GROUP, 2 * SLOTS + 1, GROUP):
        if orders % size == 0:
            best = size
    assert best > 0
    return best


def repeat(count, together, body):
    def several(i, carry):
        for k in range(together):
            body(i * together + k)
        return carry

    lax.fori_loop(0, count // together, several, 0)


def image_signs(img):
    part = lax.broadcasted_iota(jnp.int32, (1, LANES), 1) // SLOTS
    sign = jnp.ones((1, LANES), F32)
    for k in range(4):
        if SIGNS[img][k] < 0:
            sign = jnp.where(part == k, -1.0, sign)
    return sign


def kernel(
    alm_hbm, leg_hbm, fine_hbm, coarse_hbm, t_filter, w_filter, colatitude, seen,
    field_out, spec_out,
    alm, leg, fine, coarse, filt, ang, mask, lad, raised_rows, sums, send_x, recv_x, table,
    send_y, recv_y, gath_y, cols, fcols, parts, coefs_y, coefs_f, est, field_a, field_b, box,
    sem_in, sem_c, sx, rx, sy, ry, sg, rg, ss, rs,
    *, chunk, scale, pixels,
):
    orders, tiles = alm.shape[:2]
    rows = alm.shape[2]
    sims = rows // 2
    degrees = tiles * LANES
    cycles = leg.shape[1]
    blocks = recv_y.shape[0]
    chunks = recv_y.shape[1]
    groups = gath_y.shape[0]
    steps = orders // GROUP
    per_chunk = chunk // GROUP
    nblk = blocks * chunks
    width = table.shape[2]
    quad = GROUP // 2
    joint = 2 if per_chunk % 2 == 0 else 1
    me = lax.axis_index("blk")
    mine = lax.axis_index("sims")
    first = me * orders

    barrier = pltpu.get_barrier_semaphore()

    def greet_blk(o, carry):
        pl.semaphore_signal(
            barrier, inc=1, device_id={"blk": lax.rem(me + o, blocks)}, device_id_type=MESH
        )
        return carry

    def greet_sims(o, carry):
        pl.semaphore_signal(
            barrier, inc=1, device_id={"sims": lax.rem(mine + o, groups)}, device_id_type=MESH
        )
        return carry

    def start_load(n):
        part = pl.ds(n * GROUP, GROUP)
        pltpu.make_async_copy(leg_hbm.at[part], leg.at[part], sem_in.at[n % DEPTH, 0]).start()
        for s in range(sims):
            pltpu.make_async_copy(
                alm_hbm.at[part, s],
                alm.at[part, :, pl.ds(2 * s, 2), :],
                sem_in.at[n % DEPTH, 1],
            ).start()

    def wait_load(n):
        part = pl.ds(n * GROUP, GROUP)
        pltpu.make_async_copy(leg.at[part], leg.at[part], sem_in.at[n % DEPTH, 0]).wait()
        pltpu.make_async_copy(alm.at[part], alm.at[part], sem_in.at[n % DEPTH, 1]).wait()

    load_fine = pltpu.make_async_copy(fine_hbm, fine, sem_c.at[0])
    load_coarse = pltpu.make_async_copy(coarse_hbm, coarse, sem_c.at[1])

    ahead = min(DEPTH, steps)
    for n in range(ahead):
        start_load(n)
    load_fine.start()
    load_coarse.start()
    lax.fori_loop(1, blocks, greet_blk, 0)
    lax.fori_loop(1, groups, greet_sims, 0)

    degree = lax.broadcasted_iota(jnp.int32, (1, degrees), 1).astype(F32)
    lane = lax.broadcasted_iota(jnp.int32, (1, LANES), 1)
    slot = lane % SLOTS
    parity = (lane // SLOTS) % 2
    half = lane // (2 * SLOTS)
    row8 = lax.broadcasted_iota(jnp.int32, (rows, LANES), 0)
    column = lax.broadcasted_iota(jnp.int32, (rows, 1), 0)

    t_row = t_filter[...].reshape(1, degrees)
    w_row = w_filter[...].reshape(1, degrees)
    filt[0] = jnp.broadcast_to(t_row, (rows, degrees))
    filt[1] = jnp.broadcast_to(w_row, (rows, degrees))
    filt[2] = jnp.broadcast_to(degree * w_row, (rows, degrees))
    filt[3] = jnp.broadcast_to((2.0 * degree + 1.0) / jnp.maximum(2.0 * degree - 1.0, 1.0), (rows, degrees))
    filt[4] = jnp.broadcast_to(degree * (1.0 / degrees), (rows, degrees))
    filt[5] = jnp.broadcast_to(1.0 / (2.0 * degree + 1.0), (rows, degrees))

    angle = colatitude[...].reshape(1, cycles)
    cosine = jnp.cos(angle)
    cosecant = 1.0 / jnp.sin(angle)
    square_row = lax.broadcasted_iota(jnp.int32, (cycles, cycles), 0)
    square_col = lax.broadcasted_iota(jnp.int32, (cycles, cycles), 1)
    for k, value in enumerate((cosine * cosecant, cosecant, cosine)):
        spread_out = jnp.where(square_row == square_col, value, 0.0)
        ang[k] = jnp.broadcast_to(
            jnp.sum(spread_out, axis=1, keepdims=True), (cycles, LANES)
        )
    tilt_row = jnp.concatenate([cosine] * quad, axis=1)

    quarter = pixels // 4
    both = seen[...].astype(F32)
    both = jnp.where(
        lax.broadcasted_iota(jnp.int32, (rows, pixels), 0) % 2 == 0, both[0:1], both[1:2]
    )
    both = jnp.concatenate([both, jnp.zeros((rows, LANES), F32)], axis=1)
    turn_row = lax.broadcasted_iota(jnp.int32, (2 * LANES, LANES), 0)
    turn_col = lax.broadcasted_iota(jnp.int32, (2 * LANES, LANES), 1)
    turn = jnp.where(turn_row + turn_col == LANES, 1.0, 0.0).astype(BF16)
    half_seen = both.astype(BF16)
    for n in range(width // LANES):
        pixel = lane + n * LANES
        here = slice(n * LANES, (n + 1) * LANES)
        back = pixels // 2 - (n + 1) * LANES
        straight = both[:, n * LANES : (n + 1) * LANES]
        mask[0, :, here] = jnp.where(pixel <= quarter, straight, 0.0)
        mirror = jnp.dot(
            half_seen[:, back : back + 2 * LANES], turn, preferred_element_type=F32
        )
        mask[1, :, here] = jnp.where(pixel < quarter, mirror, 0.0)
        at = pixels // 2 + n * LANES
        mask[2, :, here] = jnp.where(
            (pixel > 0) & (pixel <= quarter), both[:, at : at + LANES], 0.0
        )
        back = pixels - (n + 1) * LANES
        mirror = jnp.dot(
            half_seen[:, back : back + 2 * LANES], turn, preferred_element_type=F32
        )
        mask[3, :, here] = jnp.where((pixel > 0) & (pixel < quarter), mirror, 0.0)

    def quad_orders(n, p):
        return (first + n * GROUP + 2 * (column % quad) + p).astype(F32)

    def copy_x(t, dest, source):
        return pltpu.make_async_remote_copy(
            src_ref=send_x.at[t, dest],
            dst_ref=recv_x.at[source, t],
            send_sem=sx,
            recv_sem=rx,
            device_id={"blk": dest},
            device_id_type=MESH,
        )

    for t in range(chunks):

        def block_sums(i, k):
            n = t * per_chunk + i
            for p in range(2):
                order = quad_orders(n, p)
                square = (degree * degree - order * order) * filt[3]
                ladder = jnp.where(
                    degree > order, square * lax.rsqrt(jnp.maximum(square, 1.0)), 0.0
                )
                lad[2 * n + p] = ladder * (1.0 / degrees)
                raised_rows[2 * k + p] = ladder * filt[1]
            for u in range(GROUP):
                values = jnp.concatenate(
                    [alm[n * GROUP + u, k].astype(F32) for k in range(tiles)], axis=1
                )
                raised = raised_rows[2 * k + u % 2, pl.ds(u // 2, rows, stride=0), :] * values
                lowered = pltpu.roll(raised, degrees - 1, 1)
                coefs = jnp.concatenate(
                    [filt[0] * values, filt[1] * values, filt[2] * values, lowered],
                    axis=0,
                ).astype(BF16)
                sums[pl.ds((i * GROUP + u) * cycles, cycles), 0 : 4 * rows] = lax.dot_general(
                    leg[n * GROUP + u], coefs, NT, preferred_element_type=F32
                )

        def step(i, carry):
            for k in range(joint):
                n = t * per_chunk + i * joint + k
                wait_load(n)

                @pl.when(n + ahead < steps)
                def _():
                    start_load(n + ahead)

            for k in range(joint):
                block_sums(i * joint + k, k)
            return carry

        lax.fori_loop(0, per_chunk // joint, step, 0)

        def message(dest):
            pieces = []
            for r in range(2):
                for p in range(2):
                    pieces.append(
                        sums[pl.ds(p * cycles + 2 * dest + r, SLOTS, stride=2 * cycles), :]
                    )
            turned = jnp.concatenate(pieces, axis=0).T
            order_int = first + t * chunk + 2 * slot + parity
            order = order_int.astype(F32)
            cot = jnp.where(
                half == 0, ang[0, pl.ds(2 * dest, 1), :], ang[0, pl.ds(2 * dest + 1, 1), :]
            )
            csc = jnp.where(
                half == 0, ang[1, pl.ds(2 * dest, 1), :], ang[1, pl.ds(2 * dest + 1, 1), :]
            )
            wave = turned[rows : 2 * rows]
            odd_row = row8 % 2
            rotated = jnp.where(
                odd_row == 0, -pltpu.roll(wave, rows - 1, 0), pltpu.roll(wave, 1, 0)
            ) * (csc * order)
            slopes = cot * turned[2 * rows : 3 * rows] - csc * turned[3 * rows : 4 * rows]
            weight = jnp.where(order_int > 0, 2.0, 1.0)
            out = []
            for value in (turned[:rows], rotated, slopes):
                value = jnp.where(slot < chunk // 2, value * weight, 0.0)
                swapped = pltpu.roll(value, 2 * SLOTS, 1)
                out.append(
                    jnp.where(
                        odd_row == half,
                        value,
                        jnp.where(
                            odd_row == 1, pltpu.roll(swapped, 1, 0), pltpu.roll(swapped, rows - 1, 0)
                        ),
                    )
                )
            return jnp.concatenate(out, axis=0).astype(BF16)

        if t == 0:
            pl.semaphore_wait(barrier, blocks - 1 + groups - 1)

        def send(k, carry):
            for j in range(4):
                dest = lax.rem(me + 4 * k + j, blocks)
                send_x[t, dest] = message(dest)
            for j in range(4):
                o = 4 * k + j
                dest = lax.rem(me + o, blocks)

                @pl.when(o > 0)
                def _():
                    copy_x(t, dest, me).start()

            return carry

        lax.fori_loop(0, blocks // 4, send, 0)
        recv_x[me, t] = send_x[t, me]

    load_fine.wait()
    load_coarse.wait()

    def fill(n, carry):
        table[n] = (
            fine[0] * coarse[0, pl.ds(n, 1), :] + fine[1] * coarse[1, pl.ds(n, 1), :]
        ).astype(BF16)
        return carry

    lax.fori_loop(0, nblk, fill, 0)

    def whole(ref, count, sem):
        part = ref.at[pl.ds(0, count)]
        return pltpu.make_async_copy(part, part, sem)

    whole(recv_x, blocks - 1, rx).wait()

    pieces = recv_x[...].reshape(nblk, 3 * rows, LANES)
    images = []
    for img in range(4):
        sign = image_signs(img).astype(BF16)
        images.append(
            jnp.concatenate([pieces[n] * sign for n in range(nblk)], axis=1)
        )
    stacked = jnp.concatenate(images, axis=0)
    maps = jnp.dot(
        stacked, table[...].reshape(nblk * LANES, width), preferred_element_type=F32
    )
    flows = []
    for img in range(4):
        base = img * 3 * rows
        product = mask[img] * maps[base : base + rows]
        flows.append(product * maps[base + 2 * rows : base + 3 * rows])
        flows.append(product * maps[base + rows : base + 2 * rows])
    flows = jnp.concatenate(flows, axis=0).astype(BF16)
    for n in range(nblk):
        part = lax.dot_general(flows, table[n], NT, preferred_element_type=F32)
        total = part[: 2 * rows]
        for img in range(1, 4):
            total = total + part[2 * rows * img : 2 * rows * (img + 1)] * image_signs(img)
        send_y[n // chunks, n % chunks] = (total * scale).astype(BF16)

    def copy_y(dest, source):
        return pltpu.make_async_remote_copy(
            src_ref=send_y.at[dest],
            dst_ref=recv_y.at[source],
            send_sem=sy,
            recv_sem=ry.at[source],
            device_id={"blk": dest},
            device_id_type=MESH,
        )

    def put_y(o, carry):
        copy_y(lax.rem(me + o, blocks), me).start()
        return carry

    lax.fori_loop(1, blocks, put_y, 0)
    recv_y[me] = send_y[me]

    def copy_g(o, source, group):
        return pltpu.make_async_remote_copy(
            src_ref=recv_y.at[source],
            dst_ref=gath_y.at[group, source],
            send_sem=sg,
            recv_sem=rg,
            device_id={"sims": lax.rem(mine + o, groups)},
            device_id_type=MESH,
        )

    def spread(source):
        for o in range(1, groups):
            copy_g(o, source, mine).start()

    spread(me)

    def pass_y(o, carry):
        source = lax.rem(me + o, blocks)
        copy_y(source, source).wait_recv()
        spread(source)
        return carry

    lax.fori_loop(1, blocks, pass_y, 0)

    wide = blocks * 2 * rows
    spot = lax.broadcasted_iota(jnp.int32, (rows, wide), 1)
    srow = lax.broadcasted_iota(jnp.int32, (rows, wide), 0)
    same = (spot // 2) % sims == srow % sims
    flow = (spot // rows) % 2
    mask_first = jnp.where(same & (flow == 0), 1.0, 0.0)
    mask_second = jnp.where(same & (flow == 1), jnp.where(srow < sims, 1.0, -1.0), 0.0)
    low_rows = srow < sims
    pick_row = lax.broadcasted_iota(jnp.int32, (wide, quad * cycles), 0)
    pick_col = lax.broadcasted_iota(jnp.int32, (wide, quad * cycles), 1)
    chosen = (pick_row // (2 * rows)) * 2 + pick_row % 2 == pick_col % cycles
    pick = jnp.where(chosen, 1.0, 0.0).astype(BF16)
    member = lax.broadcasted_iota(jnp.int32, (rows, quad * cycles), 1) // cycles
    for t in range(chunks):
        cols[t] = recv_y[:, t].astype(F32).reshape(wide, LANES).T

    def unpack(n):
        t = n // per_chunk
        g = n % per_chunk
        stack = []
        for p in range(2):
            for j in range(quad):
                line = p * SLOTS + quad * g + j
                real = cols[t, pl.ds(line, 1), :]
                imag = cols[t, pl.ds(line + 2 * SLOTS, 1), :]
                stack.append(jnp.where(low_rows, real, imag) * mask_first)
                stack.append(jnp.where(low_rows, imag, real) * mask_second)
        out = jnp.dot(
            jnp.concatenate(stack, axis=0).astype(BF16), pick, preferred_element_type=F32
        )
        for p in range(2):
            pieces = []
            for j in range(quad):
                base = 2 * rows * (p * quad + j)
                one = out[base : base + rows]
                two = out[base + rows : base + 2 * rows]
                tilted = (tilt_row * one).astype(BF16).astype(F32)
                for value in (tilted, one, two):
                    pieces.append(jnp.where(member == j, value, 0.0))
            coefs_y[2 * n + p] = jnp.concatenate(pieces, axis=0).astype(BF16)

    repeat(steps, joint, unpack)

    def legs(n, p):
        return jnp.concatenate(
            [leg[n * GROUP + 2 * j + p] for j in range(quad)], axis=0
        )

    def project(n):
        for p in range(2):
            out = jnp.dot(coefs_y[2 * n + p], legs(n, p), preferred_element_type=F32)
            for j in range(quad):
                base = 3 * rows * j
                order = (first + n * GROUP + 2 * j + p).astype(F32) * (1.0 / degrees)
                est[n * GROUP + 2 * j + p] = (
                    filt[4] * out[base : base + rows]
                    - lad[2 * n + p, pl.ds(j, rows, stride=0), :]
                    * pltpu.roll(out[base + rows : base + 2 * rows], 1, 1)
                    + order * out[base + 2 * rows : base + 3 * rows]
                )

    repeat(steps, joint, project)

    whole(gath_y, groups - 1, rg).wait()

    def gather_sums(b, carry):
        tilt = jnp.where(
            row8 % 2 == 0, ang[2, pl.ds(2 * b, 1), :], ang[2, pl.ds(2 * b + 1, 1), :]
        )
        for t in range(chunks):
            one = jnp.zeros((rows, LANES), F32)
            two = jnp.zeros((rows, LANES), F32)
            tilted = jnp.zeros((rows, LANES), F32)
            for o in range(groups):
                if o == 0:
                    value = recv_y[b, t].astype(F32)
                else:
                    value = gath_y[lax.rem(mine + o, groups), b, t].astype(F32)
                one = one + value[:rows]
                two = two + value[rows:]
                tilted = tilted + (tilt * value[:rows]).astype(BF16).astype(F32)
            out = []
            for value in (one, two, tilted):
                value = value + pltpu.roll(value, 2, 0)
                out.append(value + pltpu.roll(value, 4, 0))
            parts[b, t] = jnp.concatenate(out + [jnp.zeros_like(one)], axis=0)
        return carry

    lax.fori_loop(0, blocks, gather_sums, 0)
    for t in range(chunks):
        for k in range(2):
            fcols[t, k] = parts[:, t, 2 * rows * k : 2 * rows * (k + 1), :].reshape(wide, LANES).T
    head = (pick_row // 2) % sims == 0
    pick_one = jnp.where(chosen & head & ((pick_row // rows) % 2 == 0), 1.0, 0.0).astype(BF16)
    pick_two = jnp.where(chosen & head & ((pick_row // rows) % 2 == 1), 1.0, 0.0).astype(BF16)
    member_rows = member == lax.broadcasted_iota(jnp.int32, (rows, quad * cycles), 0) % quad

    def split(value):
        upper = value.astype(BF16)
        return [upper, (value - upper.astype(F32)).astype(BF16)]

    def funpack(n):
        t = n // per_chunk
        g = n % per_chunk
        ones = []
        twos = []
        for p in range(2):
            tiles_two = []
            for kind in range(2):
                tile = None
                for c in range(2):
                    for j in range(quad):
                        line = p * SLOTS + quad * g + j + 2 * SLOTS * c
                        row = fcols[t, kind, pl.ds(line, 1), :]
                        tile = row if tile is None else jnp.where(srow == quad * c + j, row, tile)
                tiles_two.append(tile)
            ones += split(tiles_two[1])
            ones += split(tiles_two[0])
            twos += split(
                jnp.where(low_rows, pltpu.roll(tiles_two[0], quad, 0), -pltpu.roll(tiles_two[0], quad, 0))
            )
        out_one = jnp.dot(jnp.concatenate(ones, axis=0), pick_one, preferred_element_type=F32)
        out_two = jnp.dot(jnp.concatenate(twos, axis=0), pick_two, preferred_element_type=F32)
        for p in range(2):
            pieces = [out_one[rows * (4 * p + k) : rows * (4 * p + k + 1)] for k in range(4)]
            pieces += [out_two[rows * (2 * p + k) : rows * (2 * p + k + 1)] for k in range(2)]
            coefs_f[2 * n + p] = jnp.concatenate(
                [jnp.where(member_rows, value, 0.0) for value in pieces], axis=0
            ).astype(BF16)

    repeat(steps, joint, funpack)

    share = degrees // groups
    span = degrees // HALVES
    shares = groups // HALVES
    every = 1.0 / (sims * groups)

    def copy_s(k, dest, source):
        part = pl.ds(k * span, span)
        return pltpu.make_async_remote_copy(
            src_ref=box.at[blocks, :, part],
            dst_ref=box.at[source, :, part],
            send_sem=ss,
            recv_sem=rs,
            device_id={"blk": dest},
            device_id_type=MESH,
        )

    span_row = lax.broadcasted_iota(jnp.int32, (rows, span), 0)
    for k in range(HALVES):
        here = slice(k * span, (k + 1) * span)
        lead = LANES if k > 0 else 0
        owner = mine // shares == k

        def project_field(n, kept):
            for p in range(2):
                tile = jnp.concatenate(
                    [
                        leg[n * GROUP + 2 * j + p, :, k * span - lead : (k + 1) * span]
                        for j in range(quad)
                    ],
                    axis=0,
                )
                out = jnp.dot(coefs_f[2 * n + p], tile, preferred_element_type=F32)
                one, two, three = [
                    out[2 * rows * q : 2 * rows * q + rows]
                    + out[2 * rows * q + rows : 2 * rows * (q + 1)]
                    for q in range(3)
                ]
                whole_field = (
                    filt[4, :, here] * one[:, lead:]
                    - lad[2 * n + p, :, here] * pltpu.roll(two, 1, 1)[:, lead:]
                    + (quad_orders(n, p) * (1.0 / degrees)) * three[:, lead:]
                )
                kept[p] = whole_field * every
                part = whole_field[:, 0:share]
                for g in range(1, shares):
                    part = jnp.where(
                        mine % shares == g, whole_field[:, g * share : (g + 1) * share], part
                    )
                for j in range(quad):
                    for c in range(2):
                        at = n * GROUP + 2 * j + p
                        line = part[quad * c + j : quad * c + j + 1]
                        if k > 0:
                            line = jnp.where(owner, line, field_out[at, c : c + 1, :])
                        field_out[at, c : c + 1, :] = line

        def centred(n, kept, p, j):
            mean = jnp.where(
                span_row < sims,
                kept[p, pl.ds(j, rows, stride=0), :],
                kept[p, pl.ds(quad + j, rows, stride=0), :],
            )
            return est[n * GROUP + 2 * j + p, :, here] - mean

        def power(n, kept, auto, cross):
            for p in range(2):
                for j in range(quad):
                    residual = centred(n, kept, p, j)
                    auto = auto + residual * residual
                    cross = cross + residual * pltpu.roll(residual, rows - 1, 0)
            return auto, cross

        def both_blocks(i, carry):
            auto, cross = carry
            project_field(jnp.minimum(2 * i + 1, steps - 1), field_b)
            auto, cross = power(2 * i, field_a, auto, cross)
            project_field(jnp.minimum(2 * i + 2, steps - 1), field_a)
            auto, cross = power(2 * i + 1, field_b, auto, cross)
            return auto, cross

        project_field(0, field_a)
        residual = jnp.where(me == 0, centred(0, field_a, 0, 0), 0.0)
        auto = -0.5 * (residual * residual)
        cross = -0.5 * (residual * pltpu.roll(residual, rows - 1, 0))
        auto, cross = lax.fori_loop(0, steps // 2, both_blocks, (auto, cross))
        if steps % 2:
            auto, cross = power(steps - 1, field_a, auto, cross)
        auto = auto + pltpu.roll(auto, sims, 0)
        cross = cross + pltpu.roll(cross, sims, 0)
        cross = jnp.where(span_row % 2 == 0, cross, pltpu.roll(cross, 1, 0))
        box[blocks, :, here] = jnp.where(span_row < sims, auto, cross) * (
            2.0 * filt[5, :, here]
        )

        def put_s(o, carry):
            copy_s(k, lax.rem(me + o, blocks), me).start()
            return carry

        lax.fori_loop(1, blocks, put_s, 0)

    box[me] = box[blocks]
    whole(box, blocks - 1, rs).wait()

    def add_s(b, value):
        return value + box[b]

    result = lax.fori_loop(0, blocks, add_s, jnp.zeros((rows, degrees), F32))
    for s in range(sims):
        spec_out[s] = jnp.concatenate([result[s : s + 1], result[sims + s : sims + s + 1]], axis=0)

    whole(recv_x, blocks - 1, sx).wait()
    whole(recv_y, blocks - 1, sy).wait()
    whole(gath_y, groups - 1, sg).wait()
    whole(box, blocks - 1, ss).wait()


def angle_tables(blocks, chunks, chunk, pixels, width):
    pixel = np.arange(width)

    def waves(orders):
        turn = 2.0 * np.pi / pixels * ((orders[:, None] * pixel[None, :]) % pixels)
        return np.cos(turn), np.sin(turn)

    even = waves(2 * np.arange(SLOTS))
    odd = waves(2 * np.arange(SLOTS) + 1)
    fine = np.stack(
        [
            np.concatenate([even[0], odd[0], -even[1], -odd[1]]),
            np.concatenate([-even[1], -odd[1], -even[0], -odd[0]]),
        ]
    )
    coarse = np.stack(waves(chunk * np.arange(blocks * chunks)))
    return fine.astype(np.float32), coarse.astype(np.float32)


def per_device(sim_alm, t_filter, wiener_filter, colatitude, legendre, pixel_mask):
    orders, sims, parts, degrees = sim_alm.shape
    cycles = legendre.shape[2]
    pixels = pixel_mask.shape[1]
    blocks = lax.axis_size("blk")
    groups = lax.axis_size("sims")
    rows = sims * parts
    tiles = degrees // LANES
    assert rows == 8 and cycles == 2 * blocks and blocks % 4 == 0
    chunk = chunk_of(orders)
    chunks = orders // chunk
    nblk = blocks * chunks
    width = pixels // 4 + LANES
    steps = orders // GROUP
    quads = 2 * steps
    wide = blocks * 2 * rows

    fine, coarse = angle_tables(blocks, chunks, chunk, pixels, width)
    leg_rows = jnp.transpose(legendre, (0, 2, 1))
    alm_tiles = jnp.transpose(
        sim_alm.reshape(orders, sims, parts, tiles, LANES), (0, 1, 3, 2, 4)
    )

    hbm = pl.BlockSpec(memory_space=pl.ANY)
    vmem = pl.BlockSpec(memory_space=pltpu.VMEM)
    dma = pltpu.SemaphoreType.DMA
    field, spectra = pl.pallas_call(
        functools.partial(kernel, chunk=chunk, scale=2.0 * math.pi / pixels, pixels=pixels),
        in_specs=[hbm, hbm, hbm, hbm, vmem, vmem, vmem, vmem],
        out_specs=[vmem, vmem],
        out_shape=[
            pltpu.VMEM((orders, 2, degrees // groups), F32),
            pltpu.VMEM((sims, 2, degrees), F32),
        ],
        scratch_shapes=[
            pltpu.VMEM((orders, tiles, rows, LANES), BF16),
            pltpu.VMEM((orders, cycles, degrees), BF16),
            pltpu.VMEM((2, LANES, width), F32),
            pltpu.VMEM((2, nblk, width), F32),
            pltpu.VMEM((6, rows, degrees), F32),
            pltpu.VMEM((3, cycles, LANES), F32),
            pltpu.VMEM((4, rows, width), F32),
            pltpu.VMEM((quads, rows, degrees), F32),
            pltpu.VMEM((4, rows, degrees), F32),
            pltpu.VMEM((2 * SLOTS * cycles, LANES), F32),
            pltpu.VMEM((chunks, blocks, 3 * rows, LANES), BF16),
            pltpu.VMEM((blocks, chunks, 3 * rows, LANES), BF16),
            pltpu.VMEM((nblk, LANES, width), BF16),
            pltpu.VMEM((blocks, chunks, 2 * rows, LANES), BF16),
            pltpu.VMEM((blocks, chunks, 2 * rows, LANES), BF16),
            pltpu.VMEM((groups, blocks, chunks, 2 * rows, LANES), BF16),
            pltpu.VMEM((chunks, LANES, wide), F32),
            pltpu.VMEM((chunks, 2, LANES, wide), F32),
            pltpu.VMEM((blocks, chunks, 4 * rows, LANES), F32),
            pltpu.VMEM((quads, 12 * rows, 4 * cycles), BF16),
            pltpu.VMEM((quads, 6 * rows, 4 * cycles), BF16),
            pltpu.VMEM((orders, rows, degrees), F32),
            pltpu.VMEM((2, rows, degrees // HALVES), F32),
            pltpu.VMEM((2, rows, degrees // HALVES), F32),
            pltpu.VMEM((1 + blocks, rows, degrees), F32),
            dma((DEPTH, 2)),
            dma((2,)),
            dma,
            dma,
            dma,
            dma((blocks,)),
            dma,
            dma,
            dma,
            dma,
        ],
        compiler_params=pltpu.CompilerParams(
            collective_id=0, has_side_effects=True, vmem_limit_bytes=VMEM_LIMIT
        ),
        name="lensing",
    )(
        alm_tiles, leg_rows, jnp.asarray(fine), jnp.asarray(coarse),
        t_filter, wiener_filter, colatitude, pixel_mask,
    )

    return field, spectra


def solution(mesh):
    placed = (P("blk", "sims", None, None), P(), P(), P(), P("blk", None, None), P("blk", None))
    return jax.shard_map(
        per_device,
        mesh=mesh,
        in_specs=placed,
        out_specs=(P("blk", None, "sims"), P("sims", None, None)),
        check_vma=False,
    )
```

```python
import functools
import math

import jax
import jax.numpy as jnp
import numpy as np
from jax import lax
from jax.experimental import pallas as pl
from jax.experimental.pallas import tpu as pltpu
from jax.sharding import PartitionSpec as P

F32 = jnp.float32
BF16 = jnp.bfloat16
LANES = 128
SLOTS = 32
GROUP = 8
DEPTH = 6
HALVES = 2
VMEM_LIMIT = 54 * 1024 * 1024
MESH = pl.DeviceIdType.MESH
NT = (((1,), (1,)), ((), ()))
SIGNS = ((1, 1, 1, 1), (1, -1, -1, 1), (1, -1, 1, -1), (1, 1, -1, -1))


def chunk_of(orders):
    best = 0
    for size in range(GROUP, 2 * SLOTS + 1, GROUP):
        if orders % size == 0:
            best = size
    assert best > 0
    return best


def repeat(count, together, body):
    def several(i, carry):
        for k in range(together):
            body(i * together + k)
        return carry

    lax.fori_loop(0, count // together, several, 0)


def image_signs(img):
    part = lax.broadcasted_iota(jnp.int32, (1, LANES), 1) // SLOTS
    sign = jnp.ones((1, LANES), F32)
    for k in range(4):
        if SIGNS[img][k] < 0:
            sign = jnp.where(part == k, -1.0, sign)
    return sign


def kernel(
    alm_hbm, leg_hbm, fine_hbm, coarse_hbm, t_filter, w_filter, colatitude, seen,
    field_out, spec_out,
    alm, leg, fine, coarse, filt, ang, mask, lad, raised_rows, sums, send_x, recv_x, table,
    send_y, recv_y, gath_y, cols, fcols, parts, coefs_y, coefs_f, est, field_a, field_b, box,
    sem_in, sem_c, sx, rx, sy, ry, sg, rg, ss, rs,
    *, chunk, scale, pixels,
):
    orders, tiles = alm.shape[:2]
    rows = alm.shape[2]
    sims = rows // 2
    degrees = tiles * LANES
    cycles = leg.shape[1]
    blocks = recv_y.shape[0]
    chunks = recv_y.shape[1]
    groups = gath_y.shape[0]
    steps = orders // GROUP
    per_chunk = chunk // GROUP
    nblk = blocks * chunks
    width = table.shape[2]
    quad = GROUP // 2
    joint = 2 if per_chunk % 2 == 0 else 1
    many = 4 if steps % 4 == 0 else 1
    me = lax.axis_index("blk")
    mine = lax.axis_index("sims")
    first = me * orders

    barrier = pltpu.get_barrier_semaphore()

    def greet_blk(o, carry):
        pl.semaphore_signal(
            barrier, inc=1, device_id={"blk": lax.rem(me + o, blocks)}, device_id_type=MESH
        )
        return carry

    def greet_sims(o, carry):
        pl.semaphore_signal(
            barrier, inc=1, device_id={"sims": lax.rem(mine + o, groups)}, device_id_type=MESH
        )
        return carry

    def start_load(n):
        part = pl.ds(n * GROUP, GROUP)
        pltpu.make_async_copy(leg_hbm.at[part], leg.at[part], sem_in.at[n % DEPTH, 0]).start()
        for s in range(sims):
            pltpu.make_async_copy(
                alm_hbm.at[part, s],
                alm.at[part, :, pl.ds(2 * s, 2), :],
                sem_in.at[n % DEPTH, 1],
            ).start()

    def wait_load(n):
        part = pl.ds(n * GROUP, GROUP)
        pltpu.make_async_copy(leg.at[part], leg.at[part], sem_in.at[n % DEPTH, 0]).wait()
        pltpu.make_async_copy(alm.at[part], alm.at[part], sem_in.at[n % DEPTH, 1]).wait()

    load_fine = pltpu.make_async_copy(fine_hbm, fine, sem_c.at[0])
    load_coarse = pltpu.make_async_copy(coarse_hbm, coarse, sem_c.at[1])

    ahead = min(DEPTH, steps)
    for n in range(ahead):
        start_load(n)
    load_fine.start()
    load_coarse.start()
    lax.fori_loop(1, blocks, greet_blk, 0)
    lax.fori_loop(1, groups, greet_sims, 0)

    degree = lax.broadcasted_iota(jnp.int32, (1, degrees), 1).astype(F32)
    lane = lax.broadcasted_iota(jnp.int32, (1, LANES), 1)
    slot = lane % SLOTS
    parity = (lane // SLOTS) % 2
    half = lane // (2 * SLOTS)
    row8 = lax.broadcasted_iota(jnp.int32, (rows, LANES), 0)
    column = lax.broadcasted_iota(jnp.int32, (rows, 1), 0)

    t_row = t_filter[...].reshape(1, degrees)
    w_row = w_filter[...].reshape(1, degrees)
    filt[0] = jnp.broadcast_to(t_row, (rows, degrees))
    filt[1] = jnp.broadcast_to(w_row, (rows, degrees))
    filt[2] = jnp.broadcast_to(degree * w_row, (rows, degrees))
    filt[3] = jnp.broadcast_to((2.0 * degree + 1.0) / jnp.maximum(2.0 * degree - 1.0, 1.0), (rows, degrees))
    filt[4] = jnp.broadcast_to(degree * (1.0 / degrees), (rows, degrees))
    filt[5] = jnp.broadcast_to(1.0 / (2.0 * degree + 1.0), (rows, degrees))

    angle = colatitude[...].reshape(1, cycles)
    cosine = jnp.cos(angle)
    cosecant = 1.0 / jnp.sin(angle)
    square_row = lax.broadcasted_iota(jnp.int32, (cycles, cycles), 0)
    square_col = lax.broadcasted_iota(jnp.int32, (cycles, cycles), 1)
    for k, value in enumerate((cosine * cosecant, cosecant, cosine)):
        spread_out = jnp.where(square_row == square_col, value, 0.0)
        ang[k] = jnp.broadcast_to(
            jnp.sum(spread_out, axis=1, keepdims=True), (cycles, LANES)
        )
    tilt_row = jnp.concatenate([cosine] * quad, axis=1)

    quarter = pixels // 4
    both = seen[...].astype(F32)
    both = jnp.where(
        lax.broadcasted_iota(jnp.int32, (rows, pixels), 0) % 2 == 0, both[0:1], both[1:2]
    )
    both = jnp.concatenate([both, jnp.zeros((rows, LANES), F32)], axis=1)
    turn_row = lax.broadcasted_iota(jnp.int32, (2 * LANES, LANES), 0)
    turn_col = lax.broadcasted_iota(jnp.int32, (2 * LANES, LANES), 1)
    turn = jnp.where(turn_row + turn_col == LANES, 1.0, 0.0).astype(BF16)
    half_seen = both.astype(BF16)
    for n in range(width // LANES):
        pixel = lane + n * LANES
        here = slice(n * LANES, (n + 1) * LANES)
        back = pixels // 2 - (n + 1) * LANES
        straight = both[:, n * LANES : (n + 1) * LANES]
        mask[0, :, here] = jnp.where(pixel <= quarter, straight, 0.0)
        mirror = jnp.dot(
            half_seen[:, back : back + 2 * LANES], turn, preferred_element_type=F32
        )
        mask[1, :, here] = jnp.where(pixel < quarter, mirror, 0.0)
        at = pixels // 2 + n * LANES
        mask[2, :, here] = jnp.where(
            (pixel > 0) & (pixel <= quarter), both[:, at : at + LANES], 0.0
        )
        back = pixels - (n + 1) * LANES
        mirror = jnp.dot(
            half_seen[:, back : back + 2 * LANES], turn, preferred_element_type=F32
        )
        mask[3, :, here] = jnp.where((pixel > 0) & (pixel < quarter), mirror, 0.0)

    def quad_orders(n, p):
        return (first + n * GROUP + 2 * (column % quad) + p).astype(F32)

    def copy_x(t, dest, source):
        return pltpu.make_async_remote_copy(
            src_ref=send_x.at[t, dest],
            dst_ref=recv_x.at[source, t],
            send_sem=sx,
            recv_sem=rx,
            device_id={"blk": dest},
            device_id_type=MESH,
        )

    for t in range(chunks):

        def block_sums(i, k):
            n = t * per_chunk + i
            for p in range(2):
                order = quad_orders(n, p)
                square = (degree * degree - order * order) * filt[3]
                ladder = jnp.where(
                    degree > order, square * lax.rsqrt(jnp.maximum(square, 1.0)), 0.0
                )
                lad[2 * n + p] = ladder * (1.0 / degrees)
                raised_rows[2 * k + p] = ladder * filt[1]
            for u in range(GROUP):
                values = jnp.concatenate(
                    [alm[n * GROUP + u, k].astype(F32) for k in range(tiles)], axis=1
                )
                raised = raised_rows[2 * k + u % 2, pl.ds(u // 2, rows, stride=0), :] * values
                lowered = pltpu.roll(raised, degrees - 1, 1)
                coefs = jnp.concatenate(
                    [filt[0] * values, filt[1] * values, filt[2] * values, lowered],
                    axis=0,
                ).astype(BF16)
                sums[pl.ds((i * GROUP + u) * cycles, cycles), 0 : 4 * rows] = lax.dot_general(
                    leg[n * GROUP + u], coefs, NT, preferred_element_type=F32
                )

        def step(i, carry):
            for k in range(joint):
                n = t * per_chunk + i * joint + k
                wait_load(n)

                @pl.when(n + ahead < steps)
                def _():
                    start_load(n + ahead)

            for k in range(joint):
                block_sums(i * joint + k, k)
            return carry

        lax.fori_loop(0, per_chunk // joint, step, 0)

        def message(dest):
            pieces = []
            for r in range(2):
                for p in range(2):
                    pieces.append(
                        sums[pl.ds(p * cycles + 2 * dest + r, SLOTS, stride=2 * cycles), :]
                    )
            turned = jnp.concatenate(pieces, axis=0).T
            order_int = first + t * chunk + 2 * slot + parity
            order = order_int.astype(F32)
            cot = jnp.where(
                half == 0, ang[0, pl.ds(2 * dest, 1), :], ang[0, pl.ds(2 * dest + 1, 1), :]
            )
            csc = jnp.where(
                half == 0, ang[1, pl.ds(2 * dest, 1), :], ang[1, pl.ds(2 * dest + 1, 1), :]
            )
            wave = turned[rows : 2 * rows]
            odd_row = row8 % 2
            rotated = jnp.where(
                odd_row == 0, -pltpu.roll(wave, rows - 1, 0), pltpu.roll(wave, 1, 0)
            ) * (csc * order)
            slopes = cot * turned[2 * rows : 3 * rows] - csc * turned[3 * rows : 4 * rows]
            weight = jnp.where(order_int > 0, 2.0, 1.0)
            out = []
            for value in (turned[:rows], rotated, slopes):
                value = jnp.where(slot < chunk // 2, value * weight, 0.0)
                swapped = pltpu.roll(value, 2 * SLOTS, 1)
                out.append(
                    jnp.where(
                        odd_row == half,
                        value,
                        jnp.where(
                            odd_row == 1, pltpu.roll(swapped, 1, 0), pltpu.roll(swapped, rows - 1, 0)
                        ),
                    )
                )
            return jnp.concatenate(out, axis=0).astype(BF16)

        if t == 0:
            pl.semaphore_wait(barrier, blocks - 1 + groups - 1)

        def send(k, carry):
            for j in range(4):
                dest = lax.rem(me + 4 * k + j, blocks)
                send_x[t, dest] = message(dest)
            for j in range(4):
                o = 4 * k + j
                dest = lax.rem(me + o, blocks)

                @pl.when(o > 0)
                def _():
                    copy_x(t, dest, me).start()

            return carry

        lax.fori_loop(0, blocks // 4, send, 0)
        recv_x[me, t] = send_x[t, me]

    load_fine.wait()
    load_coarse.wait()

    def fill(n, carry):
        table[n] = (
            fine[0] * coarse[0, pl.ds(n, 1), :] + fine[1] * coarse[1, pl.ds(n, 1), :]
        ).astype(BF16)
        return carry

    lax.fori_loop(0, nblk, fill, 0)

    def whole(ref, count, sem):
        part = ref.at[pl.ds(0, count)]
        return pltpu.make_async_copy(part, part, sem)

    whole(recv_x, blocks - 1, rx).wait()

    pieces = recv_x[...].reshape(nblk, 3 * rows, LANES)
    images = []
    for img in range(4):
        sign = image_signs(img).astype(BF16)
        images.append(
            jnp.concatenate([pieces[n] * sign for n in range(nblk)], axis=1)
        )
    stacked = jnp.concatenate(images, axis=0)
    maps = jnp.dot(
        stacked, table[...].reshape(nblk * LANES, width), preferred_element_type=F32
    )
    flows = []
    for img in range(4):
        base = img * 3 * rows
        product = mask[img] * maps[base : base + rows]
        flows.append(product * maps[base + 2 * rows : base + 3 * rows])
        flows.append(product * maps[base + rows : base + 2 * rows])
    flows = jnp.concatenate(flows, axis=0).astype(BF16)
    for n in range(nblk):
        part = lax.dot_general(flows, table[n], NT, preferred_element_type=F32)
        total = part[: 2 * rows]
        for img in range(1, 4):
            total = total + part[2 * rows * img : 2 * rows * (img + 1)] * image_signs(img)
        send_y[n // chunks, n % chunks] = (total * scale).astype(BF16)

    def copy_y(dest, source):
        return pltpu.make_async_remote_copy(
            src_ref=send_y.at[dest],
            dst_ref=recv_y.at[source],
            send_sem=sy,
            recv_sem=ry.at[source],
            device_id={"blk": dest},
            device_id_type=MESH,
        )

    def put_y(o, carry):
        copy_y(lax.rem(me + o, blocks), me).start()
        return carry

    lax.fori_loop(1, blocks, put_y, 0)
    recv_y[me] = send_y[me]

    def copy_g(o, source, group):
        return pltpu.make_async_remote_copy(
            src_ref=recv_y.at[source],
            dst_ref=gath_y.at[group, source],
            send_sem=sg,
            recv_sem=rg,
            device_id={"sims": lax.rem(mine + o, groups)},
            device_id_type=MESH,
        )

    def spread(source):
        for o in range(1, groups):
            copy_g(o, source, mine).start()

    spread(me)

    def pass_y(o, carry):
        source = lax.rem(me + o, blocks)
        copy_y(source, source).wait_recv()
        spread(source)
        return carry

    lax.fori_loop(1, blocks, pass_y, 0)

    wide = blocks * 2 * rows
    spot = lax.broadcasted_iota(jnp.int32, (rows, wide), 1)
    srow = lax.broadcasted_iota(jnp.int32, (rows, wide), 0)
    same = (spot // 2) % sims == srow % sims
    flow = (spot // rows) % 2
    mask_first = jnp.where(same & (flow == 0), 1.0, 0.0)
    mask_second = jnp.where(same & (flow == 1), jnp.where(srow < sims, 1.0, -1.0), 0.0)
    low_rows = srow < sims
    pick_row = lax.broadcasted_iota(jnp.int32, (wide, quad * cycles), 0)
    pick_col = lax.broadcasted_iota(jnp.int32, (wide, quad * cycles), 1)
    chosen = (pick_row // (2 * rows)) * 2 + pick_row % 2 == pick_col % cycles
    pick = jnp.where(chosen, 1.0, 0.0).astype(BF16)
    member = lax.broadcasted_iota(jnp.int32, (rows, quad * cycles), 1) // cycles
    for t in range(chunks):
        cols[t] = recv_y[:, t].astype(F32).reshape(wide, LANES).T

    def unpack(n):
        t = n // per_chunk
        g = n % per_chunk
        stack = []
        for p in range(2):
            for j in range(quad):
                line = p * SLOTS + quad * g + j
                real = cols[t, pl.ds(line, 1), :]
                imag = cols[t, pl.ds(line + 2 * SLOTS, 1), :]
                stack.append(jnp.where(low_rows, real, imag) * mask_first)
                stack.append(jnp.where(low_rows, imag, real) * mask_second)
        out = jnp.dot(
            jnp.concatenate(stack, axis=0).astype(BF16), pick, preferred_element_type=F32
        )
        for p in range(2):
            pieces = []
            for j in range(quad):
                base = 2 * rows * (p * quad + j)
                one = out[base : base + rows]
                two = out[base + rows : base + 2 * rows]
                tilted = (tilt_row * one).astype(BF16).astype(F32)
                for value in (tilted, one, two):
                    pieces.append(jnp.where(member == j, value, 0.0))
            coefs_y[2 * n + p] = jnp.concatenate(pieces, axis=0).astype(BF16)

    repeat(steps, many, unpack)

    def legs(n, p):
        return jnp.concatenate(
            [leg[n * GROUP + 2 * j + p] for j in range(quad)], axis=0
        )

    def project(n):
        for p in range(2):
            out = jnp.dot(coefs_y[2 * n + p], legs(n, p), preferred_element_type=F32)
            for j in range(quad):
                base = 3 * rows * j
                order = (first + n * GROUP + 2 * j + p).astype(F32) * (1.0 / degrees)
                est[n * GROUP + 2 * j + p] = (
                    filt[4] * out[base : base + rows]
                    - lad[2 * n + p, pl.ds(j, rows, stride=0), :]
                    * pltpu.roll(out[base + rows : base + 2 * rows], 1, 1)
                    + order * out[base + 2 * rows : base + 3 * rows]
                )

    repeat(steps, many, project)

    whole(gath_y, groups - 1, rg).wait()

    def gather_sums(b, carry):
        tilt = jnp.where(
            row8 % 2 == 0, ang[2, pl.ds(2 * b, 1), :], ang[2, pl.ds(2 * b + 1, 1), :]
        )
        for t in range(chunks):
            one = jnp.zeros((rows, LANES), F32)
            two = jnp.zeros((rows, LANES), F32)
            tilted = jnp.zeros((rows, LANES), F32)
            for o in range(groups):
                if o == 0:
                    value = recv_y[b, t].astype(F32)
                else:
                    value = gath_y[lax.rem(mine + o, groups), b, t].astype(F32)
                one = one + value[:rows]
                two = two + value[rows:]
                tilted = tilted + (tilt * value[:rows]).astype(BF16).astype(F32)
            out = []
            for value in (one, two, tilted):
                value = value + pltpu.roll(value, 2, 0)
                out.append(value + pltpu.roll(value, 4, 0))
            parts[b, t] = jnp.concatenate(out + [jnp.zeros_like(one)], axis=0)
        return carry

    lax.fori_loop(0, blocks, gather_sums, 0)
    for t in range(chunks):
        for k in range(2):
            fcols[t, k] = parts[:, t, 2 * rows * k : 2 * rows * (k + 1), :].reshape(wide, LANES).T
    head = (pick_row // 2) % sims == 0
    pick_one = jnp.where(chosen & head & ((pick_row // rows) % 2 == 0), 1.0, 0.0).astype(BF16)
    pick_two = jnp.where(chosen & head & ((pick_row // rows) % 2 == 1), 1.0, 0.0).astype(BF16)
    member_rows = member == lax.broadcasted_iota(jnp.int32, (rows, quad * cycles), 0) % quad

    def split(value):
        upper = value.astype(BF16)
        return [upper, (value - upper.astype(F32)).astype(BF16)]

    def funpack(n):
        t = n // per_chunk
        g = n % per_chunk
        ones = []
        twos = []
        for p in range(2):
            tiles_two = []
            for kind in range(2):
                tile = None
                for c in range(2):
                    for j in range(quad):
                        line = p * SLOTS + quad * g + j + 2 * SLOTS * c
                        row = fcols[t, kind, pl.ds(line, 1), :]
                        tile = row if tile is None else jnp.where(srow == quad * c + j, row, tile)
                tiles_two.append(tile)
            ones += split(tiles_two[1])
            ones += split(tiles_two[0])
            twos += split(
                jnp.where(low_rows, pltpu.roll(tiles_two[0], quad, 0), -pltpu.roll(tiles_two[0], quad, 0))
            )
        out_one = jnp.dot(jnp.concatenate(ones, axis=0), pick_one, preferred_element_type=F32)
        out_two = jnp.dot(jnp.concatenate(twos, axis=0), pick_two, preferred_element_type=F32)
        for p in range(2):
            pieces = [out_one[rows * (4 * p + k) : rows * (4 * p + k + 1)] for k in range(4)]
            pieces += [out_two[rows * (2 * p + k) : rows * (2 * p + k + 1)] for k in range(2)]
            coefs_f[2 * n + p] = jnp.concatenate(
                [jnp.where(member_rows, value, 0.0) for value in pieces], axis=0
            ).astype(BF16)

    repeat(steps, many, funpack)

    share = degrees // groups
    span = degrees // HALVES
    shares = groups // HALVES
    every = 1.0 / (sims * groups)

    def copy_s(k, dest, source):
        part = pl.ds(k * span, span)
        return pltpu.make_async_remote_copy(
            src_ref=box.at[blocks, :, part],
            dst_ref=box.at[source, :, part],
            send_sem=ss,
            recv_sem=rs,
            device_id={"blk": dest},
            device_id_type=MESH,
        )

    span_row = lax.broadcasted_iota(jnp.int32, (rows, span), 0)
    for k in range(HALVES):
        here = slice(k * span, (k + 1) * span)
        lead = LANES if k > 0 else 0
        owner = mine // shares == k

        def project_field(n, kept):
            for p in range(2):
                tile = jnp.concatenate(
                    [
                        leg[n * GROUP + 2 * j + p, :, k * span - lead : (k + 1) * span]
                        for j in range(quad)
                    ],
                    axis=0,
                )
                out = jnp.dot(coefs_f[2 * n + p], tile, preferred_element_type=F32)
                one, two, three = [
                    out[2 * rows * q : 2 * rows * q + rows]
                    + out[2 * rows * q + rows : 2 * rows * (q + 1)]
                    for q in range(3)
                ]
                whole_field = (
                    filt[4, :, here] * one[:, lead:]
                    - lad[2 * n + p, :, here] * pltpu.roll(two, 1, 1)[:, lead:]
                    + (quad_orders(n, p) * (1.0 / degrees)) * three[:, lead:]
                )
                kept[p] = whole_field * every
                part = whole_field[:, 0:share]
                for g in range(1, shares):
                    part = jnp.where(
                        mine % shares == g, whole_field[:, g * share : (g + 1) * share], part
                    )
                for j in range(quad):
                    for c in range(2):
                        at = n * GROUP + 2 * j + p
                        line = part[quad * c + j : quad * c + j + 1]
                        if k > 0:
                            line = jnp.where(owner, line, field_out[at, c : c + 1, :])
                        field_out[at, c : c + 1, :] = line

        def centred(n, kept, p, j):
            mean = jnp.where(
                span_row < sims,
                kept[p, pl.ds(j, rows, stride=0), :],
                kept[p, pl.ds(quad + j, rows, stride=0), :],
            )
            return est[n * GROUP + 2 * j + p, :, here] - mean

        def power(n, kept, auto, cross):
            for p in range(2):
                for j in range(quad):
                    residual = centred(n, kept, p, j)
                    auto = auto + residual * residual
                    cross = cross + residual * pltpu.roll(residual, rows - 1, 0)
            return auto, cross

        def both_blocks(i, carry):
            auto, cross = carry
            project_field(jnp.minimum(2 * i + 1, steps - 1), field_b)
            auto, cross = power(2 * i, field_a, auto, cross)
            project_field(jnp.minimum(2 * i + 2, steps - 1), field_a)
            auto, cross = power(2 * i + 1, field_b, auto, cross)
            return auto, cross

        project_field(0, field_a)
        residual = jnp.where(me == 0, centred(0, field_a, 0, 0), 0.0)
        auto = -0.5 * (residual * residual)
        cross = -0.5 * (residual * pltpu.roll(residual, rows - 1, 0))
        auto, cross = lax.fori_loop(0, steps // 2, both_blocks, (auto, cross))
        if steps % 2:
            auto, cross = power(steps - 1, field_a, auto, cross)
        auto = auto + pltpu.roll(auto, sims, 0)
        cross = cross + pltpu.roll(cross, sims, 0)
        cross = jnp.where(span_row % 2 == 0, cross, pltpu.roll(cross, 1, 0))
        box[blocks, :, here] = jnp.where(span_row < sims, auto, cross) * (
            2.0 * filt[5, :, here]
        )

        def put_s(o, carry):
            copy_s(k, lax.rem(me + o, blocks), me).start()
            return carry

        lax.fori_loop(1, blocks, put_s, 0)

    box[me] = box[blocks]
    whole(box, blocks - 1, rs).wait()

    def add_s(b, value):
        return value + box[b]

    result = lax.fori_loop(0, blocks, add_s, jnp.zeros((rows, degrees), F32))
    for s in range(sims):
        spec_out[s] = jnp.concatenate([result[s : s + 1], result[sims + s : sims + s + 1]], axis=0)

    whole(recv_x, blocks - 1, sx).wait()
    whole(recv_y, blocks - 1, sy).wait()
    whole(gath_y, groups - 1, sg).wait()
    whole(box, blocks - 1, ss).wait()


def angle_tables(blocks, chunks, chunk, pixels, width):
    pixel = np.arange(width)

    def waves(orders):
        turn = 2.0 * np.pi / pixels * ((orders[:, None] * pixel[None, :]) % pixels)
        return np.cos(turn), np.sin(turn)

    even = waves(2 * np.arange(SLOTS))
    odd = waves(2 * np.arange(SLOTS) + 1)
    fine = np.stack(
        [
            np.concatenate([even[0], odd[0], -even[1], -odd[1]]),
            np.concatenate([-even[1], -odd[1], -even[0], -odd[0]]),
        ]
    )
    coarse = np.stack(waves(chunk * np.arange(blocks * chunks)))
    return fine.astype(np.float32), coarse.astype(np.float32)


def per_device(sim_alm, t_filter, wiener_filter, colatitude, legendre, pixel_mask):
    orders, sims, parts, degrees = sim_alm.shape
    cycles = legendre.shape[2]
    pixels = pixel_mask.shape[1]
    blocks = lax.axis_size("blk")
    groups = lax.axis_size("sims")
    rows = sims * parts
    tiles = degrees // LANES
    assert rows == 8 and cycles == 2 * blocks and blocks % 4 == 0
    chunk = chunk_of(orders)
    chunks = orders // chunk
    nblk = blocks * chunks
    width = pixels // 4 + LANES
    steps = orders // GROUP
    quads = 2 * steps
    wide = blocks * 2 * rows

    fine, coarse = angle_tables(blocks, chunks, chunk, pixels, width)
    leg_rows = jnp.transpose(legendre, (0, 2, 1))
    alm_tiles = jnp.transpose(
        sim_alm.reshape(orders, sims, parts, tiles, LANES), (0, 1, 3, 2, 4)
    )

    hbm = pl.BlockSpec(memory_space=pl.ANY)
    vmem = pl.BlockSpec(memory_space=pltpu.VMEM)
    dma = pltpu.SemaphoreType.DMA
    field, spectra = pl.pallas_call(
        functools.partial(kernel, chunk=chunk, scale=2.0 * math.pi / pixels, pixels=pixels),
        in_specs=[hbm, hbm, hbm, hbm, vmem, vmem, vmem, vmem],
        out_specs=[vmem, vmem],
        out_shape=[
            pltpu.VMEM((orders, 2, degrees // groups), F32),
            pltpu.VMEM((sims, 2, degrees), F32),
        ],
        scratch_shapes=[
            pltpu.VMEM((orders, tiles, rows, LANES), BF16),
            pltpu.VMEM((orders, cycles, degrees), BF16),
            pltpu.VMEM((2, LANES, width), F32),
            pltpu.VMEM((2, nblk, width), F32),
            pltpu.VMEM((6, rows, degrees), F32),
            pltpu.VMEM((3, cycles, LANES), F32),
            pltpu.VMEM((4, rows, width), F32),
            pltpu.VMEM((quads, rows, degrees), F32),
            pltpu.VMEM((4, rows, degrees), F32),
            pltpu.VMEM((2 * SLOTS * cycles, LANES), F32),
            pltpu.VMEM((chunks, blocks, 3 * rows, LANES), BF16),
            pltpu.VMEM((blocks, chunks, 3 * rows, LANES), BF16),
            pltpu.VMEM((nblk, LANES, width), BF16),
            pltpu.VMEM((blocks, chunks, 2 * rows, LANES), BF16),
            pltpu.VMEM((blocks, chunks, 2 * rows, LANES), BF16),
            pltpu.VMEM((groups, blocks, chunks, 2 * rows, LANES), BF16),
            pltpu.VMEM((chunks, LANES, wide), F32),
            pltpu.VMEM((chunks, 2, LANES, wide), F32),
            pltpu.VMEM((blocks, chunks, 4 * rows, LANES), F32),
            pltpu.VMEM((quads, 12 * rows, 4 * cycles), BF16),
            pltpu.VMEM((quads, 6 * rows, 4 * cycles), BF16),
            pltpu.VMEM((orders, rows, degrees), F32),
            pltpu.VMEM((2, rows, degrees // HALVES), F32),
            pltpu.VMEM((2, rows, degrees // HALVES), F32),
            pltpu.VMEM((1 + blocks, rows, degrees), F32),
            dma((DEPTH, 2)),
            dma((2,)),
            dma,
            dma,
            dma,
            dma((blocks,)),
            dma,
            dma,
            dma,
            dma,
        ],
        compiler_params=pltpu.CompilerParams(
            collective_id=0, has_side_effects=True, vmem_limit_bytes=VMEM_LIMIT
        ),
        name="lensing",
    )(
        alm_tiles, leg_rows, jnp.asarray(fine), jnp.asarray(coarse),
        t_filter, wiener_filter, colatitude, pixel_mask,
    )

    return field, spectra


def solution(mesh):
    placed = (P("blk", "sims", None, None), P(), P(), P(), P("blk", None, None), P("blk", None))
    return jax.shard_map(
        per_device,
        mesh=mesh,
        in_specs=placed,
        out_specs=(P("blk", None, "sims"), P("sims", None, None)),
        check_vma=False,
    )
```
